512 devices in a mesh: section: 8 (over x, y_hi), fsdp: 64 (over z, y_lo, core).
Axes of the slice: x: 4, y: 4 (y_hi: 2, y_lo: 2; y = y_hi * 2 + y_lo), z: 16, core: 2. Of those that a mesh axis runs over, the one named last changes fastest.
Arguments:
- tokens: bfloat16 [6, 2048, 4096], P(None, 'fsdp'), may hold values from -16 to 16
- cotangent: bfloat16 [6, 2048, 4096], P(None, 'fsdp'), may hold values from -16 to 16
- order: int32 [6], replicated, may hold values from 0 to 5, each once
- w_value: bfloat16 [8, 4096, 512], P('section', 'fsdp'), may hold values from -0.09375 to 0.09375
- w_out: bfloat16 [8, 512, 4096], P('section', None, 'fsdp'), may hold values from -0.25 to 0.25
- adapter_down: bfloat16 [8, 4096, 128], P('section', 'fsdp'), may hold values from -0.09375 to 0.09375
- adapter_up: bfloat16 [8, 128, 512], P('section', None, 'fsdp'), may hold values from -0.5 to 0.5
Outputs:
- input_grads: bfloat16 [8, 6, 2048, 4096], P('section', None, 'fsdp')
- grad_down: float32 [8, 4096, 128], P('section', 'fsdp')
- grad_up: float32 [8, 128, 512], P('section', None, 'fsdp')
The draws below stay inside these ranges and needn't reach their ends.
Inputs may be any that keep to these rules, and one draw needn't show every extreme that they name: order names each microbatch 0 .. 5 exactly once.
All inputs are finite; a program needn't handle non-finite values.
Results may differ from the reference program's by a relative error of at most 0.02.
Values may be sent and summed in bfloat16 or wider, within the bound.
A program may use at most 128 MiB of HBM per device.

```python
import jax
import jax.numpy as jnp
from jax import lax

D = 4096
HV = 512
R = 128
MICRO = 6
MB = 2048
SECTIONS = 8


def with_spikes(entries, own_key, source, target, blocks, factor):
    def block_of(dim):
        return (jnp.arange(entries.shape[dim]) // (entries.shape[dim] // blocks)).reshape((-1,) + (1,) * (entries.ndim - 1 - dim))

    near = jax.random.permutation(own_key, blocks)[block_of(target)]
    second = (block_of(target) + blocks // 2) % blocks
    return jnp.where((block_of(source) == near) | (block_of(source) == second), factor * entries, entries)


def level_of(own_key, dims, pieces, least, top_value):
    gain, own = 1.0, jax.random.fold_in(own_key, 6)
    for dim, blocks in pieces:
        draws = jnp.exp(jax.random.uniform(jax.random.fold_in(own, dim), (blocks,), jnp.float32, least / len(pieces), top_value / len(pieces)))
        gain = gain * jnp.repeat(draws, dims[dim] // blocks).reshape([-1 if axis == dim else 1 for axis in range(len(dims))])
    return gain


def noise(rng, extent, width, most, cuts=(), kind=jnp.bfloat16):
    gain = level_of(rng, extent, cuts, -0.22, 0.18) if cuts else 1.0
    entries = jax.random.normal(rng, extent, jnp.float32) * width * gain
    return jnp.minimum(jnp.maximum(entries, -most), most).astype(kind)


def heavy_noise(rng, shape, spread, bound, shards, heavy, held_as=jnp.bfloat16):
    array = spread * jax.random.normal(rng, shape, jnp.float32)
    if shards:
        array = array * level_of(rng, shape, shards, -0.22, 0.18)
    return jnp.clip(with_spikes(array, jax.random.fold_in(rng, 3), *heavy), -bound, bound).astype(held_as)


def setup_inputs(seed: int = 0) -> dict:
    streams_of = jax.random.split(jax.random.key(seed), 8)
    return {
        "tokens": heavy_noise(streams_of[0], (MICRO, MB, D), 1.0, 16.0, ((1, 64),), (1, 2, 64, 4.0)),
        "cotangent": heavy_noise(streams_of[1], (MICRO, MB, D), 1.0, 16.0, ((1, 64),), (1, 2, 64, 4.0)),
        "order": jax.random.permutation(streams_of[2], MICRO).astype(jnp.int32),
        "w_value": noise(streams_of[3], (SECTIONS, D, HV), D ** -0.5, 0.09375, ((0, 8), (1, 64))),
        "w_out": noise(streams_of[4], (SECTIONS, HV, D), HV ** -0.5, 0.25, ((0, 8), (2, 64))),
        "adapter_down": noise(streams_of[5], (SECTIONS, D, R), D ** -0.5, 0.09375, ((0, 8), (1, 64))),
        "adapter_up": noise(streams_of[6], (SECTIONS, R, HV), R ** -0.5, 0.5, ((0, 8), (2, 64))),
    }


epsilon = 1e-05

def layer_forward(inputs, w_val, w_proj, a_down, a_up):
    widened = inputs.astype(jnp.float32)
    inverse = lax.rsqrt(lax.optimization_barrier(jnp.mean(widened * widened, axis=-1, keepdims=True)) + epsilon)
    normed = (widened * inverse).astype(jnp.bfloat16)
    low = jnp.dot(normed, a_down, preferred_element_type=jnp.float32).astype(jnp.bfloat16)
    values = (jnp.dot(normed, w_val, preferred_element_type=jnp.float32) + jnp.dot(low, a_up, preferred_element_type=jnp.float32)).astype(jnp.bfloat16)
    outputs = (widened + jnp.dot(values, w_proj, preferred_element_type=jnp.float32)).astype(jnp.bfloat16)
    return (outputs, normed, low, inverse)

def layer_backward(inputs, inverse, upstream, w_val, w_proj, a_down, a_up):
    d_values = jnp.dot(upstream, w_proj.T, preferred_element_type=jnp.float32).astype(jnp.bfloat16)
    d_low = jnp.dot(d_values, a_up.T, preferred_element_type=jnp.float32).astype(jnp.bfloat16)
    d_normed = jnp.dot(d_values, w_val.T, preferred_element_type=jnp.float32) + jnp.dot(d_low, a_down.T, preferred_element_type=jnp.float32)
    widened = inputs.astype(jnp.float32)
    project = lax.optimization_barrier(jnp.mean(d_normed * widened, axis=-1, keepdims=True))
    d_inputs = upstream.astype(jnp.float32) + inverse * (d_normed - widened * inverse * inverse * project)
    return (d_inputs.astype(jnp.bfloat16), d_values, d_low)

def reference(tokens, cotangent, order, w_value, w_out, adapter_down, adapter_up):
    current = tokens[order].reshape(MICRO * MB, D)
    stored = []
    for section_index in range(SECTIONS):
        stored.append(current)
        current = layer_forward(current, w_value[section_index], w_out[section_index], adapter_down[section_index], adapter_up[section_index])[0]
    upstream = cotangent[order].reshape(MICRO * MB, D)
    grads_in = [None] * SECTIONS
    down_grads = [None] * SECTIONS
    up_grads = [None] * SECTIONS
    for section_index in reversed(range(SECTIONS)):
        inputs = stored[section_index]
        unused, normed, low, inverse = layer_forward(inputs, w_value[section_index], w_out[section_index], adapter_down[section_index], adapter_up[section_index])
        d_inputs, d_values, d_low = layer_backward(inputs, inverse, upstream, w_value[section_index], w_out[section_index], adapter_down[section_index], adapter_up[section_index])
        down_grads[section_index] = jnp.dot(normed.T, d_low, preferred_element_type=jnp.float32)
        up_grads[section_index] = jnp.dot(low.T, d_values, preferred_element_type=jnp.float32)
        grads_in[section_index] = d_inputs.reshape(MICRO, MB, D)
        upstream = d_inputs
    return (jnp.stack(grads_in), jnp.stack(down_grads), jnp.stack(up_grads))
```

```python
import functools

import jax
import jax.numpy as jnp
from jax import lax
from jax.experimental import pallas as pl
from jax.experimental.pallas import tpu as pltpu
from jax.sharding import PartitionSpec as P

EPS = 1e-05
MESH = pl.DeviceIdType.MESH
F32 = jnp.float32
BF16 = jnp.bfloat16
NT = (((1,), (1,)), ((), ()))
TN = (((0,), (0,)), ((), ()))
NY = 4
PIECES = 4


def dot(a, b):
    return jnp.dot(a, b, preferred_element_type=F32)


def dot_nt(a, b):
    return lax.dot_general(a, b, NT, preferred_element_type=F32)


class Dims:
    def __init__(self, mesh, rows, width, hv):
        self.nx = mesh.shape["section"] // 2
        self.nz = mesh.shape["fsdp"] // 4
        self.nh = self.nz // 2
        self.rows = rows
        self.d = width
        self.hv = hv
        self.hb = hv // 128
        self.off_out = 64 * self.hb
        self.off_down = 128 * self.hb
        self.off_up = self.off_down + 64
        self.shard = self.off_up + 16
        tiles = self.shard // 16
        self.rp = (tiles * 351 // 1000 + 1) * 16 if tiles < 37 else 208
        self.half = max((tiles + 1) // 2 * 16, self.rp)
        self.qa = self.rp + (tiles - self.rp // 16) // 2 * 16


def kernel(dm, shard, tok, cot, out, gout, buf, xs, ns, iv, lo, gs, dv, dl, up, dn, rr, rc, s1, t1, t2, v1, v2, s2,
           zb, zr, yr, ss, cs, fr, fs, br, bs, os, gsm, zrr):
    nx, nz, nh, d_all, hv, hb = dm.nx, dm.nz, dm.nh, dm.d, dm.hv, dm.hb
    sec = lax.axis_index("section")
    fid = lax.axis_index("fsdp")
    x = sec // 2
    yh = sec % 2
    z = fid // 4
    y = yh * 2 + (fid // 2) % 2
    c = fid % 2
    yp, ym, yo = (y + 1) % NY, (y + NY - 1) % NY, (y + 2) % NY
    zp, zm = (z + 1) % nz, (z + nz - 1) % nz

    def dev(x_, y_, z_, c_):
        return (x_ * 2 + y_ // 2, z_ * 4 + (y_ % 2) * 2 + c_)

    def slot(y_, z_, c_):
        return (y_ // 2) * (4 * nz) + z_ * 4 + (y_ % 2) * 2 + c_

    d_zp, d_zm = dev(x, y, zp, c), dev(x, y, zm, c)
    d_yp, d_ym, d_yo = dev(x, yp, z, c), dev(x, ym, z, c), dev(x, yo, z, c)
    d_sib = dev(x, y, z, 1 - c)
    d_xp, d_xm = dev(x + 1, y, z, c), dev(x - 1, y, z, c)

    def send(src, dst, ssem, rsem, to):
        pltpu.make_async_remote_copy(
            src_ref=src, dst_ref=dst, send_sem=ssem, recv_sem=rsem, device_id=to, device_id_type=MESH
        ).start()

    def got(ref, rsem):
        pltpu.make_async_remote_copy(
            src_ref=ref, dst_ref=ref, send_sem=rsem, recv_sem=rsem, device_id=d_sib, device_id_type=MESH
        ).wait_recv()

    def left(ref, ssem):
        pltpu.make_async_remote_copy(
            src_ref=ref, dst_ref=ref, send_sem=ssem, recv_sem=ssem, device_id=d_sib, device_id_type=MESH
        ).wait_send()

    barrier = pltpu.get_barrier_semaphore()

    def greet(to):
        pl.semaphore_signal(barrier, inc=1, device_id=to, device_id_type=MESH)

    for to in (d_sib, d_yp, d_ym, d_yo):
        greet(to)

    def greet_z(i, _):
        greet(dev(x, y, (z + i) % nz, c))
        return _

    lax.fori_loop(1, nz, greet_z, 0)

    greet(dev((x + nx - 1) % nx, y, z, c))
    greet(dev((x + 1) % nx, y, z, c))
    pl.semaphore_wait(barrier, 4 + nz - 1 + 2)

    rows, rp, half, qa = dm.shard, dm.rp, dm.half, dm.qa

    def part(s, r0, r1):
        return buf.at[s, pl.ds(r0, r1 - r0), :]

    def to_sib(s, r0, r1):
        send(part(s, r0, r1), part(s, r0, r1), cs.at[0], cs.at[1], d_sib)

    def move(s, r0, r1, ssem, rsem, to):
        send(part(s, r0, r1), part(s, r0, r1), ssem, rsem, to)

    me = slot(y, z, c)
    own = buf.at[me]
    send(shard, own, ss.at[0], zr.at[0, 1, 0], d_zp)
    if nh > 1:
        send(shard, own, ss.at[1], zr.at[1, 1, 0], d_zm)
    send(shard, own, ss.at[4], yr.at[0, 0], d_yp)
    send(shard, own, ss.at[11], yr.at[0, 1], d_ym)
    send(shard, own, cs.at[0], cs.at[1], d_sib)
    local = pltpu.make_async_copy(shard, own, cs.at[2])
    local.start()

    def send_p(s, kind, dist_of):
        for way, (ps, to) in enumerate(((2, d_zp), (3, d_zm))):
            if way == 0 or nh > 1:
                move(s, 0, rp, ss.at[ps], zr.at[way, dist_of, kind], to)

    s_m, s_p, s_o = slot(ym, z, c), slot(yp, z, c), slot(yo, z, c)
    got(part(s_m, 0, rows), yr.at[0, 0])
    move(s_m, 0, half, ss.at[5], yr.at[0, 2], d_yp)
    send_p(s_m, 2, 1)
    to_sib(s_m, 0, rows)
    got(part(s_p, 0, rows), yr.at[0, 1])
    move(s_p, half, rows, ss.at[6], yr.at[0, 3], d_ym)
    send_p(s_p, 1, 1)
    to_sib(s_p, 0, rows)

    def z_from(way, d):
        return (z + nz - d) % nz if way == 0 else (z + d) % nz

    def e_of(way, d):
        return d if way == 0 else nh + d

    def limit(way):
        return nh if way == 0 else nh - 1

    def z_shard(way, d):
        s = slot(y, z_from(way, d), c)
        e = e_of(way, d)
        got(part(s, 0, rows), zr.at[way, d, 0])

        @pl.when(d < limit(way))
        def _():
            move(s, 0, rows, ss.at[way], zr.at[way, d + 1, 0], (d_zp, d_zm)[way])

        move(s, rp, rows, ss.at[7], yr.at[e, 0], d_yp)
        move(s, rp, rows, ss.at[8], yr.at[e, 1], d_ym)
        to_sib(s, 0, rows)

    def z_parts(way, d):
        for kind, col in ((2, ym), (1, yp), (3, yo)):
            s = slot(col, z_from(way, d), c)
            got(part(s, 0, rp), zr.at[way, d, kind])

            @pl.when(d < limit(way))
            def _(s=s, kind=kind):
                move(s, 0, rp, ss.at[2 + way], zr.at[way, d + 1, kind], (d_zp, d_zm)[way])

            to_sib(s, 0, rp)

    def y_near(way, d):
        e, zz = e_of(way, d), z_from(way, d)
        a, b = slot(ym, zz, c), slot(yp, zz, c)
        got(part(a, rp, rows), yr.at[e, 0])
        move(a, rp, qa, ss.at[9], yr.at[e, 2], d_yp)
        to_sib(a, rp, rows)
        got(part(b, rp, rows), yr.at[e, 1])
        move(b, qa, rows, ss.at[10], yr.at[e, 3], d_ym)
        to_sib(b, rp, rows)

    def y_far(way, d):
        e, zz = e_of(way, d), z_from(way, d)
        s = slot(yo, zz, c)
        got(part(s, rp, qa), yr.at[e, 2])
        to_sib(s, rp, qa)
        got(part(s, qa, rows), yr.at[e, 3])
        to_sib(s, qa, rows)

    def gather_step(d, carry):
        for way in (0, 1):
            pl.when(d <= limit(way))(functools.partial(z_shard, way, d))

        @pl.when(d == 1)
        def _():
            got(part(s_o, 0, half), yr.at[0, 2])
            send_p(s_o, 3, 1)
            to_sib(s_o, 0, half)
            got(part(s_o, half, rows), yr.at[0, 3])
            to_sib(s_o, half, rows)

        for way in (0, 1):
            pl.when(d <= limit(way))(functools.partial(z_parts, way, d))
        for way in (0, 1):
            pl.when((d > 1) & (d <= limit(way) + 1))(functools.partial(y_near, way, d - 1))
        for way in (0, 1):
            pl.when((d > 2) & (d <= limit(way) + 2))(functools.partial(y_far, way, d - 2))
        return carry

    lax.fori_loop(1, nh + 3, gather_step, 0)

    local.wait()
    half_all = buf.at[pl.ds(0, 4 * nz)]
    got(half_all, cs.at[1])
    left(half_all, cs.at[0])

    def span(n, r):
        return buf.at[pl.ds(0, n), pl.ds(0, r), :]

    left(span(nh, rows), ss.at[0])
    left(span(3 * nh, rp), ss.at[2])
    if nh > 1:
        left(span(nh - 1, rows), ss.at[1])
        left(span(3 * (nh - 1), rp), ss.at[3])
    left(span(1, rows), ss.at[4])
    left(span(1, rows), ss.at[11])
    left(span(1, half), ss.at[5])
    left(span(1, rows - half), ss.at[6])
    left(span(nz - 1, rows - rp), ss.at[7])
    left(span(nz - 1, rows - rp), ss.at[8])
    left(span(nz - 1, qa - rp), ss.at[9])
    left(span(nz - 1, rows - qa), ss.at[10])

    for l in range(2):
        raw = buf[pl.ds(l * 4 * nz, 4 * nz), pl.ds(dm.off_up, 16), :].astype(F32)
        up[l] = raw[:, :8, :].reshape(hv, 128).astype(BF16)

    @pl.when(x == 0)
    def _():
        for u in range(3):
            xs[0, u] = tok[u]

    @pl.when(x == nx - 1)
    def _():
        for u in range(3):
            gs[2, u] = cot[u]

    tokens = dm.rows

    def block(l, k, off):
        return buf[pl.ds(l * 4 * nz + 4 * k, 4), pl.ds(off, 64), :].reshape(256, 128)

    def w_in(l, k):
        return jnp.concatenate([block(l, k, 64 * b) for b in range(hb)] + [block(l, k, dm.off_down)], axis=1)

    def w_back(l, k):
        return jnp.concatenate([block(l, k, dm.off_out + 64 * b) for b in range(hb)], axis=1)

    def cols(k):
        return pl.ds(256 * k, 256)

    width = d_all // PIECES
    per_piece = nz // PIECES

    def piece(ref, i, u, p):
        return ref.at[i, u, :, pl.ds(width * p, width)]

    def lanes(v):
        return v[:, :128] + v[:, 128:]

    def run_forward(u):
        @pl.when(x > 0)
        def _():
            for p in range(PIECES):
                got(piece(xs, 0, u, p), fr.at[u, p])

        def layer(l, carry):
            total = jnp.zeros((tokens, 128), F32)
            for k in range(nz):
                v = xs[l, u, :, cols(k)].astype(F32)
                total = total + lanes(v * v)
            inv = lax.rsqrt(jnp.sum(total, axis=-1, keepdims=True) * (1.0 / d_all) + EPS)
            iv[l, u] = jnp.broadcast_to(inv, (tokens, 128))
            for k in range(nz):
                ns[l, u, :, cols(k)] = (xs[l, u, :, cols(k)].astype(F32) * inv).astype(BF16)
            acc = jnp.zeros((tokens, hv + 128), F32)
            for k in range(nz):
                acc = acc + dot(ns[l, u, :, cols(k)], w_in(l, k))
            low = acc[:, hv:].astype(BF16)
            lo[l, u] = low
            val = (acc[:, :hv] + dot_nt(low, up[l])).astype(BF16)

            @pl.when(l + x < nx)
            def _():
                for p in range(PIECES):
                    for k in range(p * per_piece, (p + 1) * per_piece):
                        o = xs[l, u, :, cols(k)].astype(F32) + dot_nt(val, w_back(l, k))
                        xs[l + 1, u, :, cols(k)] = o.astype(BF16)
                    for q in ((p - 1,) if p < PIECES - 1 else (p - 1, p)):
                        if q >= 0:

                            @pl.when(l == 1)
                            def _(q=q):
                                send(piece(xs, 2, u, q), piece(xs, 0, u, q), fs.at[u, q], fr.at[u, q], d_xp)

            return carry

        lax.fori_loop(0, 2, layer, 0)

    def run_backward(u):
        @pl.when(x < nx - 1)
        def _():
            for p in range(PIECES):
                got(piece(gs, 2, u, p), br.at[u, p])

        def layer(i, carry):
            l = 1 - i
            acc = jnp.zeros((tokens, hv), F32)
            for k in range(nz):
                acc = acc + dot(gs[l + 1, u, :, cols(k)], w_back(l, k))
            dvb = acc.astype(BF16)
            dv[l, u] = dvb
            dlb = dot(dvb, up[l]).astype(BF16)
            dl[l, u] = dlb
            both = jnp.concatenate([dvb, dlb], axis=1)
            m = jnp.zeros((tokens, 128), F32)
            for k in range(nz):
                g = dot_nt(both, w_in(l, k))
                dn[:, cols(k)] = g
                m = m + lanes(g * xs[l, u, :, cols(k)].astype(F32))
            mean = jnp.sum(m, axis=-1, keepdims=True) * (1.0 / d_all)
            inv = iv[l, u][:, :1]
            scale = inv * inv * mean
            for p in range(PIECES):
                for k in range(p * per_piece, (p + 1) * per_piece):
                    g = dn[:, cols(k)] - xs[l, u, :, cols(k)].astype(F32) * scale
                    gs[l, u, :, cols(k)] = (gs[l + 1, u, :, cols(k)].astype(F32) + inv * g).astype(BF16)
            for p in range(PIECES):

                @pl.when((l == 0) & (x > 0))
                def _(p=p):
                    send(piece(gs, 0, u, p), piece(gs, 2, u, p), bs.at[u, p], br.at[u, p], d_xm)

            @pl.when(l == yh)
            def _():
                pltpu.make_async_copy(gs.at[l, u], out.at[3 * yh + u], os.at[0, u]).start()

            @pl.when(l != yh)
            def _():
                send(gs.at[l, u], out.at[3 * yh + u], os.at[1, u], os.at[2, u], d_yo)

            return carry

        lax.fori_loop(0, 2, layer, 0)

    last = x // (nx - 1)

    def turn(t, carry):
        u = last * (t // 2) + (1 - last) * (t % 3)
        back = last * (t % 2) + (1 - last) * (t // 3)

        @pl.when(back == 0)
        def _():
            run_forward(u)

        @pl.when(back == 1)
        def _():
            run_backward(u)

        return carry

    lax.fori_loop(0, 6, turn, 0)

    def adapter_grads(l, carry):
        dl_all = dl[l].reshape(3 * tokens, 128)
        lo_all = lo[l].reshape(3 * tokens, 128)
        for k in range(nz):
            n_k = ns[l, :, :, cols(k)].reshape(3 * tokens, 256)
            g = lax.dot_general(n_k, dl_all, TN, preferred_element_type=F32).astype(BF16)
            for q in range(4):
                rr[2 * l + q // 2, k, q % 2, pl.ds(0, 64), :] = g[64 * q : 64 * q + 64]
        dv_all = dv[l].reshape(3 * tokens, hv)
        g = lax.dot_general(dv_all, lo_all, TN, preferred_element_type=F32).reshape(nz, 4, 8, 128)
        for q in range(4):
            g_q = g[:, q]
            padded = jnp.concatenate([g_q, jnp.zeros_like(g_q)], axis=1).astype(BF16)
            rr[2 * l + q // 2, :, q % 2, pl.ds(64, 16), :] = padded
        return carry

    lax.fori_loop(0, 2, adapter_grads, 0)

    send(rr.at[:, :, 1 - c], rc, gsm.at[0], gsm.at[1], d_sib)
    got(rc, gsm.at[1])

    def add_core(i, carry):
        a, b = i // nz, i % nz
        s1[a, b] = (rr[a, b, c].astype(F32) + rc[a, b].astype(F32)).astype(BF16)
        return carry

    lax.fori_loop(0, 4 * nz, add_core, 0)
    lo_z, hi_z = pl.ds(0, nh), pl.ds(nh, nh)
    send(s1.at[yo, lo_z], t1, gsm.at[2], gsm.at[3], d_yp)
    send(s1.at[yo, hi_z], t2, gsm.at[4], gsm.at[5], d_ym)
    got(t1, gsm.at[3])

    def add_near(i, carry):
        s1[yp, i] = (s1[yp, i].astype(F32) + t1[i].astype(F32)).astype(BF16)
        return carry

    lax.fori_loop(0, nh, add_near, 0)
    send(s1.at[yp], v1, gsm.at[6], gsm.at[7], d_yp)
    got(t2, gsm.at[5])

    def add_far(i, carry):
        s1[ym, nh + i] = (s1[ym, nh + i].astype(F32) + t2[i].astype(F32)).astype(BF16)
        return carry

    lax.fori_loop(0, nh, add_far, 0)
    send(s1.at[ym], v2, gsm.at[8], gsm.at[9], d_ym)
    got(v1, gsm.at[7])
    got(v2, gsm.at[9])

    def add_y(i, carry):
        s2[i] = (s1[y, i].astype(F32) + v1[i].astype(F32) + v2[i].astype(F32)).astype(BF16)
        return carry

    lax.fori_loop(0, nz, add_y, 0)

    def z_send(i, carry):
        zz = (z + i) % nz
        send(s2.at[zz], zb.at[i], gsm.at[10], zrr.at[i], dev(x, y, zz, c))
        return carry

    lax.fori_loop(1, nz, z_send, 0)

    def z_add(i, acc):
        got(zb.at[i], zrr.at[i])
        return acc + zb[i].astype(F32)

    gout[...] = lax.fori_loop(1, nz, z_add, s2[z].astype(F32))

    left(zb.at[pl.ds(0, nz - 1)], gsm.at[10])
    left(rc, gsm.at[0])
    left(t1, gsm.at[2])
    left(t2, gsm.at[4])
    left(v1, gsm.at[6])
    left(v2, gsm.at[8])
    for u in range(3):
        for p in range(PIECES):

            @pl.when(x < nx - 1)
            def _(u=u, p=p):
                left(piece(xs, 2, u, p), fs.at[u, p])

            @pl.when(x > 0)
            def _(u=u, p=p):
                left(piece(gs, 0, u, p), bs.at[u, p])

        pltpu.make_async_copy(gs.at[0, u], out.at[3 * yh + u], os.at[0, u]).wait()
        left(gs.at[0, u], os.at[1, u])
        got(out.at[3 * (1 - yh) + u], os.at[2, u])


def run_all(dm, shard, tok, cot):
    nz, d, hv, t = dm.nz, dm.d, dm.hv, dm.rows
    vm = pltpu.VMEM
    dma = pltpu.SemaphoreType.DMA
    return pl.pallas_call(
        functools.partial(kernel, dm),
        out_shape=(
            jax.ShapeDtypeStruct((6, t, d), BF16),
            jax.ShapeDtypeStruct((80, 128), F32),
        ),
        in_specs=[pl.BlockSpec(memory_space=vm)] * 3,
        out_specs=(pl.BlockSpec(memory_space=pl.ANY), pl.BlockSpec(memory_space=vm)),
        scratch_shapes=[
            vm((8 * nz, dm.shard, 128), BF16),
            vm((3, 3, t, d), BF16),
            vm((2, 3, t, d), BF16),
            vm((2, 3, t, 128), F32),
            vm((2, 3, t, 128), BF16),
            vm((3, 3, t, d), BF16),
            vm((2, 3, t, hv), BF16),
            vm((2, 3, t, 128), BF16),
            vm((2, hv, 128), BF16),
            vm((t, d), F32),
            vm((4, nz, 2, 80, 128), BF16),
            vm((4, nz, 80, 128), BF16),
            vm((4, nz, 80, 128), BF16),
            vm((dm.nh, 80, 128), BF16),
            vm((dm.nh, 80, 128), BF16),
            vm((nz, 80, 128), BF16),
            vm((nz, 80, 128), BF16),
            vm((nz, 80, 128), BF16),
            vm((nz, 80, 128), BF16),
            dma((2, dm.nh + 2, 4)),
            dma((nz, 4)),
            dma((12,)),
            dma((3,)),
            dma((3, PIECES)),
            dma((3, PIECES)),
            dma((3, PIECES)),
            dma((3, PIECES)),
            dma((3, 3)),
            dma((11,)),
            dma((nz,)),
        ],
        compiler_params=pltpu.CompilerParams(
            collective_id=0, has_side_effects=True, vmem_limit_bytes=60 * 1024 * 1024
        ),
        name="relay",
    )(shard, tok, cot)


def lane_blocks(a):
    return jnp.swapaxes(a.reshape(a.shape[0], -1, 128), 0, 1).reshape(-1, 128)


def solution(mesh):
    def body(tokens, cotangent, order, w_value, w_out, adapter_down, adapter_up):
        dm = Dims(mesh, tokens.shape[1], tokens.shape[2], w_value.shape[2])
        up_t = adapter_up[0].T
        shard = jnp.concatenate(
            [
                lane_blocks(w_value[0]),
                lane_blocks(w_out[0].T),
                adapter_down[0],
                up_t,
                jnp.zeros_like(up_t),
            ],
            axis=0,
        )
        half = lax.axis_index("section") % 2
        mine = lax.dynamic_slice(order, (3 * half,), (3,))
        dx, grads = run_all(dm, shard, tokens[mine], cotangent[mine])
        return (dx[None], grads[:64][None], grads[64:72].T[None])

    return jax.shard_map(
        body,
        mesh=mesh,
        in_specs=(
            P(None, "fsdp", None),
            P(None, "fsdp", None),
            P(),
            P("section", "fsdp", None),
            P("section", None, "fsdp"),
            P("section", "fsdp", None),
            P("section", None, "fsdp"),
        ),
        out_specs=(
            P("section", None, "fsdp", None),
            P("section", "fsdp", None),
            P("section", None, "fsdp"),
        ),
        check_vma=False,
    )
```

```python
import functools

import jax
import jax.numpy as jnp
from jax import lax
from jax.experimental import pallas as pl
from jax.experimental.pallas import tpu as pltpu
from jax.sharding import PartitionSpec as P

EPS = 1e-05
MESH = pl.DeviceIdType.MESH
F32 = jnp.float32
BF16 = jnp.bfloat16
NT = (((1,), (1,)), ((), ()))
TN = (((0,), (0,)), ((), ()))
NY = 4
PIECES = 4


def dot(a, b):
    return jnp.dot(a, b, preferred_element_type=F32)


def dot_nt(a, b):
    return lax.dot_general(a, b, NT, preferred_element_type=F32)


class Dims:
    def __init__(self, mesh, rows, width, hv):
        self.nx = mesh.shape["section"] // 2
        self.nz = mesh.shape["fsdp"] // 4
        self.nh = self.nz // 2
        self.rows = rows
        self.d = width
        self.hv = hv
        self.hb = hv // 128
        self.off_out = 64 * self.hb
        self.off_down = 128 * self.hb
        self.off_up = self.off_down + 64
        self.shard = self.off_up + 16
        tiles = self.shard // 16
        self.rp = (tiles * 351 // 1000 + 1) * 16 if tiles < 37 else 208
        self.half = max((tiles + 1) // 2 * 16, self.rp)
        self.qa = self.rp + (tiles - self.rp // 16) // 2 * 16


def kernel(dm, order, wv, wo, ad, au, tok, cot, out, gdown, gup, shard, stage, buf, xs, nt, iv, raw, lo, gs, dv, dl,
           up, rr, rc, s1, t1, t2, v1, v2, s2, zb, zr, yr, ss, cs, fr, fs, br, bs, os, gsm, zrr):
    nx, nz, nh, d_all, hv, hb = dm.nx, dm.nz, dm.nh, dm.d, dm.hv, dm.hb
    sec = lax.axis_index("section")
    fid = lax.axis_index("fsdp")
    x = sec // 2
    yh = sec % 2
    z = fid // 4
    y = yh * 2 + (fid // 2) % 2
    c = fid % 2
    yp, ym, yo = (y + 1) % NY, (y + NY - 1) % NY, (y + 2) % NY
    zp, zm = (z + 1) % nz, (z + nz - 1) % nz

    def dev(x_, y_, z_, c_):
        return (x_ * 2 + y_ // 2, z_ * 4 + (y_ % 2) * 2 + c_)

    def slot(y_, z_, c_):
        return (y_ // 2) * (4 * nz) + z_ * 4 + (y_ % 2) * 2 + c_

    d_zp, d_zm = dev(x, y, zp, c), dev(x, y, zm, c)
    d_yp, d_ym, d_yo = dev(x, yp, z, c), dev(x, ym, z, c), dev(x, yo, z, c)
    d_sib = dev(x, y, z, 1 - c)
    d_xp, d_xm = dev(x + 1, y, z, c), dev(x - 1, y, z, c)

    def send(src, dst, ssem, rsem, to):
        pltpu.make_async_remote_copy(
            src_ref=src, dst_ref=dst, send_sem=ssem, recv_sem=rsem, device_id=to, device_id_type=MESH
        ).start()

    def got(ref, rsem):
        pltpu.make_async_remote_copy(
            src_ref=ref, dst_ref=ref, send_sem=rsem, recv_sem=rsem, device_id=d_sib, device_id_type=MESH
        ).wait_recv()

    def left(ref, ssem):
        pltpu.make_async_remote_copy(
            src_ref=ref, dst_ref=ref, send_sem=ssem, recv_sem=ssem, device_id=d_sib, device_id_type=MESH
        ).wait_send()

    @pl.when(x == 0)
    def _():
        pltpu.make_async_copy(tok, stage, cs.at[3]).start()

    @pl.when(x == nx - 1)
    def _():
        pltpu.make_async_copy(cot, stage, cs.at[3]).start()

    for b in range(hb):
        shard[pl.ds(64 * b, 64)] = wv[:, 128 * b : 128 * b + 128]
        turned = wo[128 * b : 128 * b + 128, :].astype(F32).T
        shard[pl.ds(dm.off_out + 64 * b, 64)] = turned.astype(BF16)
    shard[pl.ds(dm.off_down, 64)] = ad[...]
    turned = au[...].astype(F32).T
    shard[pl.ds(dm.off_up, 16)] = jnp.concatenate([turned, jnp.zeros_like(turned)], axis=0).astype(BF16)

    barrier = pltpu.get_barrier_semaphore()

    def greet(to):
        pl.semaphore_signal(barrier, inc=1, device_id=to, device_id_type=MESH)

    for to in (d_sib, d_yp, d_ym, d_yo):
        greet(to)

    def greet_z(i, _):
        greet(dev(x, y, (z + i) % nz, c))
        return _

    lax.fori_loop(1, nz, greet_z, 0)

    greet(dev((x + nx - 1) % nx, y, z, c))
    greet(dev((x + 1) % nx, y, z, c))
    pl.semaphore_wait(barrier, 4 + nz - 1 + 2)

    rows, rp, half, qa = dm.shard, dm.rp, dm.half, dm.qa

    def part(s, r0, r1):
        return buf.at[s, pl.ds(r0, r1 - r0), :]

    def to_sib(s, r0, r1):
        send(part(s, r0, r1), part(s, r0, r1), cs.at[0], cs.at[1], d_sib)

    def move(s, r0, r1, ssem, rsem, to):
        send(part(s, r0, r1), part(s, r0, r1), ssem, rsem, to)

    me = slot(y, z, c)
    own = buf.at[me]
    send(shard, own, ss.at[0], zr.at[0, 1, 0], d_zp)
    if nh > 1:
        send(shard, own, ss.at[1], zr.at[1, 1, 0], d_zm)
    send(shard, own, ss.at[4], yr.at[0, 0], d_yp)
    send(shard, own, ss.at[11], yr.at[0, 1], d_ym)
    send(shard, own, cs.at[0], cs.at[1], d_sib)
    local = pltpu.make_async_copy(shard, own, cs.at[2])
    local.start()

    @pl.when(x == 0)
    def _():
        pltpu.make_async_copy(tok, stage, cs.at[3]).wait()
        for u in range(3):
            xs[0, u] = stage[order[3 * yh + u]]

    @pl.when(x == nx - 1)
    def _():
        pltpu.make_async_copy(cot, stage, cs.at[3]).wait()
        for u in range(3):
            gs[2, u] = stage[order[3 * yh + u]]

    def send_p(s, kind, dist_of):
        for way, (ps, to) in enumerate(((2, d_zp), (3, d_zm))):
            if way == 0 or nh > 1:
                move(s, 0, rp, ss.at[ps], zr.at[way, dist_of, kind], to)

    s_m, s_p, s_o = slot(ym, z, c), slot(yp, z, c), slot(yo, z, c)
    got(part(s_m, 0, rows), yr.at[0, 0])
    move(s_m, 0, half, ss.at[5], yr.at[0, 2], d_yp)
    send_p(s_m, 2, 1)
    to_sib(s_m, 0, rows)
    got(part(s_p, 0, rows), yr.at[0, 1])
    move(s_p, half, rows, ss.at[6], yr.at[0, 3], d_ym)
    send_p(s_p, 1, 1)
    to_sib(s_p, 0, rows)

    def z_from(way, d):
        return (z + nz - d) % nz if way == 0 else (z + d) % nz

    def e_of(way, d):
        return d if way == 0 else nh + d

    def limit(way):
        return nh if way == 0 else nh - 1

    def z_shard(way, d):
        s = slot(y, z_from(way, d), c)
        e = e_of(way, d)
        got(part(s, 0, rows), zr.at[way, d, 0])

        @pl.when(d < limit(way))
        def _():
            move(s, 0, rows, ss.at[way], zr.at[way, d + 1, 0], (d_zp, d_zm)[way])

        move(s, rp, rows, ss.at[7], yr.at[e, 0], d_yp)
        move(s, rp, rows, ss.at[8], yr.at[e, 1], d_ym)
        to_sib(s, 0, rows)

    def z_parts(way, d):
        for kind, col in ((2, ym), (1, yp), (3, yo)):
            s = slot(col, z_from(way, d), c)
            got(part(s, 0, rp), zr.at[way, d, kind])

            @pl.when(d < limit(way))
            def _(s=s, kind=kind):
                move(s, 0, rp, ss.at[2 + way], zr.at[way, d + 1, kind], (d_zp, d_zm)[way])

            to_sib(s, 0, rp)

    def y_near(way, d):
        e, zz = e_of(way, d), z_from(way, d)
        a, b = slot(ym, zz, c), slot(yp, zz, c)
        got(part(a, rp, rows), yr.at[e, 0])
        move(a, rp, qa, ss.at[9], yr.at[e, 2], d_yp)
        to_sib(a, rp, rows)
        got(part(b, rp, rows), yr.at[e, 1])
        move(b, qa, rows, ss.at[10], yr.at[e, 3], d_ym)
        to_sib(b, rp, rows)

    def y_far(way, d):
        e, zz = e_of(way, d), z_from(way, d)
        s = slot(yo, zz, c)
        got(part(s, rp, qa), yr.at[e, 2])
        to_sib(s, rp, qa)
        got(part(s, qa, rows), yr.at[e, 3])
        to_sib(s, qa, rows)

    def gather_step(d, carry):
        for way in (0, 1):
            pl.when(d <= limit(way))(functools.partial(z_shard, way, d))

        @pl.when(d == 1)
        def _():
            got(part(s_o, 0, half), yr.at[0, 2])
            send_p(s_o, 3, 1)
            to_sib(s_o, 0, half)
            got(part(s_o, half, rows), yr.at[0, 3])
            to_sib(s_o, half, rows)

        for way in (0, 1):
            pl.when(d <= limit(way))(functools.partial(z_parts, way, d))
        for way in (0, 1):
            pl.when((d > 1) & (d <= limit(way) + 1))(functools.partial(y_near, way, d - 1))
        for way in (0, 1):
            pl.when((d > 2) & (d <= limit(way) + 2))(functools.partial(y_far, way, d - 2))
        return carry

    lax.fori_loop(1, nh + 3, gather_step, 0)

    local.wait()
    half_all = buf.at[pl.ds(0, 4 * nz)]
    got(half_all, cs.at[1])
    left(half_all, cs.at[0])

    def span(n, r):
        return buf.at[pl.ds(0, n), pl.ds(0, r), :]

    left(span(nh, rows), ss.at[0])
    left(span(3 * nh, rp), ss.at[2])
    if nh > 1:
        left(span(nh - 1, rows), ss.at[1])
        left(span(3 * (nh - 1), rp), ss.at[3])
    left(span(1, rows), ss.at[4])
    left(span(1, rows), ss.at[11])
    left(span(1, half), ss.at[5])
    left(span(1, rows - half), ss.at[6])
    left(span(nz - 1, rows - rp), ss.at[7])
    left(span(nz - 1, rows - rp), ss.at[8])
    left(span(nz - 1, qa - rp), ss.at[9])
    left(span(nz - 1, rows - qa), ss.at[10])

    for l in range(2):
        packed = buf[pl.ds(l * 4 * nz, 4 * nz), pl.ds(dm.off_up, 16), :].astype(F32)
        up[l] = packed[:, :8, :].reshape(hv, 128).astype(BF16)

    tokens = dm.rows

    def block(l, k, off):
        return buf[pl.ds(l * 4 * nz + 4 * k, 4), pl.ds(off, 64), :].reshape(256, 128)

    def w_in(l, k):
        return jnp.concatenate([block(l, k, 64 * b) for b in range(hb)] + [block(l, k, dm.off_down)], axis=1)

    def w_back(l, k):
        return jnp.concatenate([block(l, k, dm.off_out + 64 * b) for b in range(hb)], axis=1)

    def cols(k):
        return pl.ds(256 * k, 256)

    width = d_all // PIECES
    per_piece = nz // PIECES

    def piece(ref, i, u, p):
        return ref.at[i, u, :, pl.ds(width * p, width)]

    def lanes(v):
        return v[:, :128] + v[:, 128:]

    def run_forward(u):
        for l in range(2):
            total = jnp.zeros((tokens, 128), F32)
            acc = jnp.zeros((tokens, hv + 128), F32)
            for p in range(PIECES):
                if l == 0:

                    @pl.when(x > 0)
                    def _(p=p):
                        got(piece(xs, 0, u, p), fr.at[u, p])

                for k in range(p * per_piece, (p + 1) * per_piece):
                    v = xs[l, u, :, cols(k)]
                    acc = acc + dot(v, w_in(l, k))
                    v = v.astype(F32)
                    total = total + lanes(v * v)
            inv = lax.rsqrt(jnp.sum(total, axis=-1, keepdims=True) * (1.0 / d_all) + EPS)
            iv[l, u] = jnp.broadcast_to(inv, (tokens, 128))
            raw[l, u] = acc
            acc = acc * inv
            low = acc[:, hv:].astype(BF16)
            lo[l, u] = low
            val = (acc[:, :hv] + dot_nt(low, up[l])).astype(BF16)

            def outputs(l=l, val=val):
                for p in range(PIECES):
                    for k in range(p * per_piece, (p + 1) * per_piece):
                        o = xs[l, u, :, cols(k)].astype(F32) + dot_nt(val, w_back(l, k))
                        xs[l + 1, u, :, cols(k)] = o.astype(BF16)
                    if l == 1:
                        for q in (p - 1,) if p < PIECES - 1 else (p - 1, p):
                            if q >= 0:
                                send(piece(xs, 2, u, q), piece(xs, 0, u, q), fs.at[u, q], fr.at[u, q], d_xp)

            if l == 0:
                outputs()
            else:
                pl.when(x < nx - 1)(outputs)

    def run_backward(u):
        for l in (1, 0):
            acc = jnp.zeros((tokens, hv), F32)
            for p in range(PIECES):
                if l == 1:

                    @pl.when(x < nx - 1)
                    def _(p=p):
                        got(piece(gs, 2, u, p), br.at[u, p])

                for k in range(p * per_piece, (p + 1) * per_piece):
                    acc = acc + dot(gs[l + 1, u, :, cols(k)], w_back(l, k))
            dvb = acc.astype(BF16)
            dv[l, u] = dvb
            dlb = dot(dvb, up[l]).astype(BF16)
            dl[l, u] = dlb
            both = jnp.concatenate([dvb, dlb], axis=1)
            mean = jnp.sum(both.astype(F32) * raw[l, u], axis=-1, keepdims=True) * (1.0 / d_all)
            inv = iv[l, u][:, :1]
            scale = inv * inv * mean
            for p in range(PIECES):
                for k in range(p * per_piece, (p + 1) * per_piece):
                    g = dot_nt(both, w_in(l, k)) - xs[l, u, :, cols(k)].astype(F32) * scale
                    gs[l, u, :, cols(k)] = (gs[l + 1, u, :, cols(k)].astype(F32) + inv * g).astype(BF16)
                if l == 0:
                    for q in (p - 1,) if p < PIECES - 1 else (p - 1, p):
                        if q >= 0:

                            @pl.when(x > 0)
                            def _(q=q):
                                send(piece(gs, 0, u, q), piece(gs, 2, u, q), bs.at[u, q], br.at[u, q], d_xm)

            @pl.when(yh == l)
            def _(l=l):
                pltpu.make_async_copy(gs.at[l, u], out.at[3 * yh + u], os.at[0, u]).start()

            @pl.when(yh != l)
            def _(l=l):
                send(gs.at[l, u], out.at[3 * yh + u], os.at[1, u], os.at[2, u], d_yo)

    pad = jnp.zeros((128 - 3 * tokens, 128), BF16)

    def turn_normed():
        def layer(l, carry):
            inv = iv[l].reshape(3 * tokens, 128)[:, :1]
            for k in range(2 * nz):
                lane = pl.ds(128 * k, 128)
                n_k = xs[l, :, :, lane].reshape(3 * tokens, 128).astype(F32) * inv
                nt[l, lane, :] = jnp.concatenate([n_k.astype(BF16), pad], axis=0).T
            return carry

        lax.fori_loop(0, 2, layer, 0)

    last = x // (nx - 1)

    def turn(t, carry):
        u = last * ((t // 2) % 3) + (1 - last) * (t % 4)
        kind = last * (t % 2 + 2 * (t // 6)) + (1 - last) * (t // 4 + 2 * ((t % 4) // 3))

        @pl.when(kind == 0)
        def _():
            run_forward(u)

        @pl.when(kind == 1)
        def _():
            run_backward(u)

        @pl.when(kind == 2)
        def _():
            turn_normed()

        return carry

    lax.fori_loop(0, 7, turn, 0)

    def adapter_grads(l, carry):
        dl_all = jnp.concatenate([dl[l].reshape(3 * tokens, 128), pad], axis=0)
        lo_all = lo[l].reshape(3 * tokens, 128)
        for k in range(nz):
            g = dot(nt[l, cols(k), :], dl_all).astype(BF16)
            for q in range(4):
                rr[2 * l + q // 2, k, q % 2, pl.ds(0, 64), :] = g[64 * q : 64 * q + 64]
        dv_all = dv[l].reshape(3 * tokens, hv)
        g = lax.dot_general(dv_all, lo_all, TN, preferred_element_type=F32).reshape(nz, 4, 8, 128)
        for q in range(4):
            g_q = g[:, q]
            padded = jnp.concatenate([g_q, jnp.zeros_like(g_q)], axis=1).astype(BF16)
            rr[2 * l + q // 2, :, q % 2, pl.ds(64, 16), :] = padded
        return carry

    lax.fori_loop(0, 2, adapter_grads, 0)

    halves = ((0, 48), (48, 32))
    lo_z, hi_z = pl.ds(0, nh), pl.ds(nh, nh)

    def rows_of(h):
        return pl.ds(*halves[h])

    for h in range(2):
        r = rows_of(h)
        send(rr.at[:, :, 1 - c, r, :], rc.at[:, :, r, :], gsm.at[h, 0], gsm.at[h, 1], d_sib)
    for h in range(2):
        r = rows_of(h)
        got(rc.at[:, :, r, :], gsm.at[h, 1])

        def add_core(i, carry, r=r):
            s1[i, :, r, :] = (rr[i, :, c, r, :].astype(F32) + rc[i, :, r, :].astype(F32)).astype(BF16)
            return carry

        lax.fori_loop(0, NY, add_core, 0)
        send(s1.at[yo, lo_z, r, :], t1.at[:, r, :], gsm.at[h, 2], gsm.at[h, 3], d_yp)
        send(s1.at[yo, hi_z, r, :], t2.at[:, r, :], gsm.at[h, 4], gsm.at[h, 5], d_ym)
    for h in range(2):
        r = rows_of(h)
        got(t1.at[:, r, :], gsm.at[h, 3])
        s1[yp, lo_z, r, :] = (s1[yp, lo_z, r, :].astype(F32) + t1[:, r, :].astype(F32)).astype(BF16)
        got(t2.at[:, r, :], gsm.at[h, 5])
        s1[ym, hi_z, r, :] = (s1[ym, hi_z, r, :].astype(F32) + t2[:, r, :].astype(F32)).astype(BF16)
        send(s1.at[yp, :, r, :], v1.at[:, r, :], gsm.at[h, 6], gsm.at[h, 7], d_yp)
        send(s1.at[ym, :, r, :], v2.at[:, r, :], gsm.at[h, 8], gsm.at[h, 9], d_ym)
    for h in range(2):
        r = rows_of(h)
        got(v1.at[:, r, :], gsm.at[h, 7])
        got(v2.at[:, r, :], gsm.at[h, 9])
        total = s1[y, :, r, :].astype(F32) + v1[:, r, :].astype(F32) + v2[:, r, :].astype(F32)
        s2[:, r, :] = total.astype(BF16)

        def z_send(i, carry, h=h, r=r):
            zz = (z + i) % nz
            send(s2.at[zz, r, :], zb.at[i, r, :], gsm.at[h, 10], zrr.at[h, i], dev(x, y, zz, c))
            return carry

        lax.fori_loop(1, nz, z_send, 0)

    def z_sum(h):
        r = rows_of(h)

        def z_add(i, acc):
            got(zb.at[i, r, :], zrr.at[h, i])
            return acc + zb[i, r, :].astype(F32)

        return lax.fori_loop(1, nz, z_add, s2[z, r, :].astype(F32))

    top, bottom = z_sum(0), z_sum(1)
    gdown[pl.ds(0, 48)] = top
    gdown[pl.ds(48, 16)] = bottom[:16]
    gup[...] = bottom[16:24].T

    for h in range(2):
        r = rows_of(h)
        left(zb.at[pl.ds(0, nz - 1), r, :], gsm.at[h, 10])
        left(rc.at[:, :, r, :], gsm.at[h, 0])
        left(t1.at[:, r, :], gsm.at[h, 2])
        left(t2.at[:, r, :], gsm.at[h, 4])
        left(v1.at[:, r, :], gsm.at[h, 6])
        left(v2.at[:, r, :], gsm.at[h, 8])
    for u in range(3):
        for p in range(PIECES):

            @pl.when(x < nx - 1)
            def _(u=u, p=p):
                left(piece(xs, 2, u, p), fs.at[u, p])

            @pl.when(x > 0)
            def _(u=u, p=p):
                left(piece(gs, 0, u, p), bs.at[u, p])

        pltpu.make_async_copy(gs.at[0, u], out.at[3 * yh + u], os.at[0, u]).wait()
        left(gs.at[0, u], os.at[1, u])
        got(out.at[3 * (1 - yh) + u], os.at[2, u])


def run_all(dm, order, wv, wo, ad, au, tok, cot):
    nz, d, hv, t = dm.nz, dm.d, dm.hv, dm.rows
    vm = pltpu.VMEM
    dma = pltpu.SemaphoreType.DMA
    in_vmem = pl.BlockSpec(memory_space=vm)
    anywhere = pl.BlockSpec(memory_space=pl.ANY)
    return pl.pallas_call(
        functools.partial(kernel, dm),
        out_shape=(
            jax.ShapeDtypeStruct((6, t, d), BF16),
            jax.ShapeDtypeStruct((64, 128), F32),
            jax.ShapeDtypeStruct((128, 8), F32),
        ),
        in_specs=[pl.BlockSpec(memory_space=pltpu.SMEM)] + [in_vmem] * 4 + [anywhere] * 2,
        out_specs=(anywhere, in_vmem, in_vmem),
        scratch_shapes=[
            vm((dm.shard, 128), BF16),
            vm((6, t, d), BF16),
            vm((8 * nz, dm.shard, 128), BF16),
            vm((3, 3, t, d), BF16),
            vm((2, d, 128), BF16),
            vm((2, 3, t, 128), F32),
            vm((2, 3, t, hv + 128), F32),
            vm((2, 3, t, 128), BF16),
            vm((3, 3, t, d), BF16),
            vm((2, 3, t, hv), BF16),
            vm((2, 3, t, 128), BF16),
            vm((2, hv, 128), BF16),
            vm((4, nz, 2, 80, 128), BF16),
            vm((4, nz, 80, 128), BF16),
            vm((4, nz, 80, 128), BF16),
            vm((dm.nh, 80, 128), BF16),
            vm((dm.nh, 80, 128), BF16),
            vm((nz, 80, 128), BF16),
            vm((nz, 80, 128), BF16),
            vm((nz, 80, 128), BF16),
            vm((nz, 80, 128), BF16),
            dma((2, dm.nh + 2, 4)),
            dma((nz, 4)),
            dma((12,)),
            dma((4,)),
            dma((3, PIECES)),
            dma((3, PIECES)),
            dma((3, PIECES)),
            dma((3, PIECES)),
            dma((3, 3)),
            dma((2, 11)),
            dma((2, nz)),
        ],
        compiler_params=pltpu.CompilerParams(
            collective_id=0, has_side_effects=True, vmem_limit_bytes=60 * 1024 * 1024
        ),
        name="relay",
    )(order, wv, wo, ad, au, tok, cot)


def solution(mesh):
    def body(tokens, cotangent, order, w_value, w_out, adapter_down, adapter_up):
        dm = Dims(mesh, tokens.shape[1], tokens.shape[2], w_value.shape[2])
        dx, down, up = run_all(
            dm, order, w_value[0], w_out[0], adapter_down[0], adapter_up[0], tokens, cotangent
        )
        return (dx[None], down[None], up[None])

    return jax.shard_map(
        body,
        mesh=mesh,
        in_specs=(
            P(None, "fsdp", None),
            P(None, "fsdp", None),
            P(),
            P("section", "fsdp", None),
            P("section", None, "fsdp"),
            P("section", "fsdp", None),
            P("section", None, "fsdp"),
        ),
        out_specs=(
            P("section", None, "fsdp", None),
            P("section", "fsdp", None),
            P("section", None, "fsdp"),
        ),
        check_vma=False,
    )
```

```python
import functools

import jax
import jax.numpy as jnp
from jax import lax
from jax.experimental import pallas as pl
from jax.experimental.pallas import tpu as pltpu
from jax.sharding import PartitionSpec as P

EPS = 1e-05
MESH = pl.DeviceIdType.MESH
F32 = jnp.float32
BF16 = jnp.bfloat16
NT = (((1,), (1,)), ((), ()))
TN = (((0,), (0,)), ((), ()))
NY = 4
PIECES = 4


def dot(a, b):
    return jnp.dot(a, b, preferred_element_type=F32)


def dot_nt(a, b):
    return lax.dot_general(a, b, NT, preferred_element_type=F32)


class Dims:
    def __init__(self, mesh, rows, width, hv):
        self.nx = mesh.shape["section"] // 2
        self.nz = mesh.shape["fsdp"] // 4
        self.nh = self.nz // 2
        self.rows = rows
        self.d = width
        self.hv = hv
        self.hb = hv // 128
        self.off_out = 64 * self.hb
        self.off_down = 128 * self.hb
        self.off_up = self.off_down + 64
        self.shard = self.off_up + 16
        tiles = self.shard // 16
        self.rp = (tiles * 351 // 1000 + 1) * 16 if tiles < 37 else 208
        self.half = max((tiles + 1) // 2 * 16, self.rp)
        self.qa = self.rp + (tiles - self.rp // 16) // 2 * 16


def kernel(dm, order, wv, wo, ad, au, tok, cot, out, gdown, gup, shard, stage, buf, xs, nt, iv, raw, pre, lo, gs, dv, dl,
           up, rr, rc, s1, t1, t2, v1, v2, s2, zb, zr, yr, ss, cs, fr, fs, br, bs, os, gsm, zrr):
    nx, nz, nh, d_all, hv, hb = dm.nx, dm.nz, dm.nh, dm.d, dm.hv, dm.hb
    sec = lax.axis_index("section")
    fid = lax.axis_index("fsdp")
    x = sec // 2
    yh = sec % 2
    z = fid // 4
    y = yh * 2 + (fid // 2) % 2
    c = fid % 2
    yp, ym, yo = (y + 1) % NY, (y + NY - 1) % NY, (y + 2) % NY
    zp, zm = (z + 1) % nz, (z + nz - 1) % nz

    def dev(x_, y_, z_, c_):
        return (x_ * 2 + y_ // 2, z_ * 4 + (y_ % 2) * 2 + c_)

    def slot(y_, z_, c_):
        return (y_ // 2) * (4 * nz) + z_ * 4 + (y_ % 2) * 2 + c_

    d_zp, d_zm = dev(x, y, zp, c), dev(x, y, zm, c)
    d_yp, d_ym, d_yo = dev(x, yp, z, c), dev(x, ym, z, c), dev(x, yo, z, c)
    d_sib = dev(x, y, z, 1 - c)
    d_xp, d_xm = dev(x + 1, y, z, c), dev(x - 1, y, z, c)

    def send(src, dst, ssem, rsem, to):
        pltpu.make_async_remote_copy(
            src_ref=src, dst_ref=dst, send_sem=ssem, recv_sem=rsem, device_id=to, device_id_type=MESH
        ).start()

    def got(ref, rsem):
        pltpu.make_async_remote_copy(
            src_ref=ref, dst_ref=ref, send_sem=rsem, recv_sem=rsem, device_id=d_sib, device_id_type=MESH
        ).wait_recv()

    def left(ref, ssem):
        pltpu.make_async_remote_copy(
            src_ref=ref, dst_ref=ref, send_sem=ssem, recv_sem=ssem, device_id=d_sib, device_id_type=MESH
        ).wait_send()

    @pl.when(x == 0)
    def _():
        pltpu.make_async_copy(tok, stage, cs.at[3]).start()

    @pl.when(x == nx - 1)
    def _():
        pltpu.make_async_copy(cot, stage, cs.at[3]).start()

    for b in range(hb):
        shard[pl.ds(64 * b, 64)] = wv[:, 128 * b : 128 * b + 128]
        shard[pl.ds(dm.off_out + 64 * b, 64)] = wo[:, 128 * b : 128 * b + 128]
    shard[pl.ds(dm.off_down, 64)] = ad[...]
    turned = au[...].astype(F32)
    shard[pl.ds(dm.off_up, 16)] = jnp.concatenate([turned, jnp.zeros_like(turned)], axis=0).astype(BF16)

    barrier = pltpu.get_barrier_semaphore()

    def greet(to):
        pl.semaphore_signal(barrier, inc=1, device_id=to, device_id_type=MESH)

    d_xs = dev((x + nx - 1) % nx, y, z, c), dev((x + 1) % nx, y, z, c)
    peers = (d_sib, d_yp, d_ym, d_zp, d_zm, *d_xs)
    for to in peers:
        greet(to)
    pl.semaphore_wait(barrier, len(peers))

    rows, rp, half, qa = dm.shard, dm.rp, dm.half, dm.qa

    def part(s, r0, r1):
        return buf.at[s, pl.ds(r0, r1 - r0), :]

    def to_sib(s, r0, r1):
        send(part(s, r0, r1), part(s, r0, r1), cs.at[0], cs.at[1], d_sib)

    def move(s, r0, r1, ssem, rsem, to):
        send(part(s, r0, r1), part(s, r0, r1), ssem, rsem, to)

    me = slot(y, z, c)
    own = buf.at[me]
    send(shard, own, ss.at[0], zr.at[0, 1, 0], d_zp)
    send(shard, own, ss.at[1], zr.at[1, 1, 0], d_zm)
    send(shard, own, ss.at[4], yr.at[0, 0], d_yp)
    send(shard, own, ss.at[11], yr.at[0, 1], d_ym)
    send(shard, own, cs.at[0], cs.at[1], d_sib)
    local = pltpu.make_async_copy(shard, own, cs.at[2])
    local.start()

    @pl.when(x == 0)
    def _():
        pltpu.make_async_copy(tok, stage, cs.at[3]).wait()
        for u in range(3):
            xs[0, u] = stage[order[3 * yh + u]]

    @pl.when(x == nx - 1)
    def _():
        pltpu.make_async_copy(cot, stage, cs.at[3]).wait()
        for u in range(3):
            gs[2, u] = stage[order[3 * yh + u]]

    def send_p(s, kind, dist_of):
        for way, (ps, to) in enumerate(((2, d_zp), (3, d_zm))):
            move(s, 0, rp, ss.at[ps], zr.at[way, dist_of, kind], to)

    s_m, s_p, s_o = slot(ym, z, c), slot(yp, z, c), slot(yo, z, c)
    got(part(s_m, 0, rows), yr.at[0, 0])
    move(s_m, 0, half, ss.at[5], yr.at[0, 2], d_yp)
    send_p(s_m, 2, 1)
    to_sib(s_m, 0, rows)
    got(part(s_p, 0, rows), yr.at[0, 1])
    move(s_p, half, rows, ss.at[6], yr.at[0, 3], d_ym)
    send_p(s_p, 1, 1)
    to_sib(s_p, 0, rows)

    def z_from(way, d):
        return (z + nz - d) % nz if way == 0 else (z + d) % nz

    def e_of(way, d):
        return d if way == 0 else nh + d

    def limit(way):
        return nh if way == 0 else nh - 1

    def limit_p(way):
        return nh - 1 if way == 0 else nh

    def z_shard(way, d):
        s = slot(y, z_from(way, d), c)
        e = e_of(way, d)
        got(part(s, 0, rows), zr.at[way, d, 0])

        @pl.when(d < limit(way))
        def _():
            move(s, 0, rows, ss.at[way], zr.at[way, d + 1, 0], (d_zp, d_zm)[way])

        move(s, rp, rows, ss.at[7], yr.at[e, 0], d_yp)
        move(s, rp, rows, ss.at[8], yr.at[e, 1], d_ym)
        to_sib(s, 0, rows)

    def z_parts(way, d):
        for kind, col in ((2, ym), (1, yp), (3, yo)):
            s = slot(col, z_from(way, d), c)
            got(part(s, 0, rp), zr.at[way, d, kind])

            @pl.when(d < limit_p(way))
            def _(s=s, kind=kind):
                move(s, 0, rp, ss.at[2 + way], zr.at[way, d + 1, kind], (d_zp, d_zm)[way])

            to_sib(s, 0, rp)

    def y_near(way, d):
        e, zz = e_of(way, d), z_from(way, d)
        a, b = slot(ym, zz, c), slot(yp, zz, c)
        got(part(a, rp, rows), yr.at[e, 0])
        move(a, rp, qa, ss.at[9], yr.at[e, 2], d_yp)
        to_sib(a, rp, rows)
        got(part(b, rp, rows), yr.at[e, 1])
        move(b, qa, rows, ss.at[10], yr.at[e, 3], d_ym)
        to_sib(b, rp, rows)

    def y_far(way, d):
        e, zz = e_of(way, d), z_from(way, d)
        s = slot(yo, zz, c)
        got(part(s, rp, qa), yr.at[e, 2])
        to_sib(s, rp, qa)
        got(part(s, qa, rows), yr.at[e, 3])
        to_sib(s, qa, rows)

    def gather_step(d, carry):
        for way in (0, 1):
            pl.when(d <= limit(way))(functools.partial(z_shard, way, d))

        @pl.when(d == 1)
        def _():
            got(part(s_o, 0, half), yr.at[0, 2])
            send_p(s_o, 3, 1)
            to_sib(s_o, 0, half)
            got(part(s_o, half, rows), yr.at[0, 3])
            to_sib(s_o, half, rows)

        for way in (0, 1):
            pl.when(d <= limit_p(way))(functools.partial(z_parts, way, d))
        for way in (0, 1):
            pl.when((d > 1) & (d <= limit(way) + 1))(functools.partial(y_near, way, d - 1))
        for way in (0, 1):
            pl.when((d > 2) & (d <= limit(way) + 2))(functools.partial(y_far, way, d - 2))
        return carry

    lax.fori_loop(1, nh + 3, gather_step, 0)

    local.wait()
    half_all = buf.at[pl.ds(0, 4 * nz)]
    got(half_all, cs.at[1])
    left(half_all, cs.at[0])

    def span(n, r):
        return buf.at[pl.ds(0, n), pl.ds(0, r), :]

    left(span(nh, rows), ss.at[0])
    left(span(nh - 1, rows), ss.at[1])
    left(span(3 * (nh - 1), rp), ss.at[2])
    left(span(3 * nh, rp), ss.at[3])
    left(span(1, rows), ss.at[4])
    left(span(1, rows), ss.at[11])
    left(span(1, half), ss.at[5])
    left(span(1, rows - half), ss.at[6])
    left(span(nz - 1, rows - rp), ss.at[7])
    left(span(nz - 1, rows - rp), ss.at[8])
    left(span(nz - 1, qa - rp), ss.at[9])
    left(span(nz - 1, rows - qa), ss.at[10])

    for l in range(2):
        packed = buf[pl.ds(l * 4 * nz, 4 * nz), pl.ds(dm.off_up, 16), :].astype(F32)
        up[l] = packed[:, :8, :].reshape(hv, 128).astype(BF16)

    tokens = dm.rows

    def block(l, k, off):
        return buf[pl.ds(l * 4 * nz + 4 * k, 4), pl.ds(off, 64), :].reshape(256, 128)

    def w_in(l, k):
        return jnp.concatenate([block(l, k, 64 * b) for b in range(hb)] + [block(l, k, dm.off_down)], axis=1)

    def w_back(l, k):
        return jnp.concatenate([block(l, k, dm.off_out + 64 * b) for b in range(hb)], axis=1)

    def cols(k):
        return pl.ds(256 * k, 256)

    width = d_all // PIECES
    per_piece = nz // PIECES

    def piece(ref, i, u, p):
        return ref.at[i, u, :, pl.ds(width * p, width)]

    def lanes(v):
        return v[:, :128] + v[:, 128:]

    def run_forward(u):
        for l in range(2):
            total = jnp.zeros((tokens, 128), F32)
            acc = jnp.zeros((tokens, hv + 128), F32)
            for p in range(PIECES):
                if l == 0:

                    @pl.when(x > 0)
                    def _(p=p):
                        got(piece(xs, 0, u, p), fr.at[u, p])

                for k in range(p * per_piece, (p + 1) * per_piece):
                    v = xs[l, u, :, cols(k)]
                    acc = acc + dot(v, w_in(l, k))
                    v = v.astype(F32)
                    total = total + lanes(v * v)
            inv = lax.rsqrt(jnp.sum(total, axis=-1, keepdims=True) * (1.0 / d_all) + EPS)
            iv[l, u] = jnp.broadcast_to(inv, (tokens, 128))
            raw[l, u] = acc
            acc = acc * inv
            low = acc[:, hv:].astype(BF16)
            lo[l, u] = low
            val = (acc[:, :hv] + dot_nt(low, up[l])).astype(BF16)

            def outputs(l=l, val=val):
                for p in range(PIECES):
                    for k in range(p * per_piece, (p + 1) * per_piece):
                        o = xs[l, u, :, cols(k)].astype(F32) + dot_nt(val, w_back(l, k))
                        xs[l + 1, u, :, cols(k)] = o.astype(BF16)
                    if l == 1:
                        for q in (p - 1,) if p < PIECES - 1 else (p - 1, p):
                            if q >= 0:
                                send(piece(xs, 2, u, q), piece(xs, 0, u, q), fs.at[u, q], fr.at[u, q], d_xp)

            if l == 0:
                outputs()
            else:
                pl.when(x < nx - 1)(outputs)

    def adapter_side(l, u, acc):
        dvb = acc.astype(BF16)
        dv[l, u] = dvb
        dlb = dot(dvb, up[l]).astype(BF16)
        dl[l, u] = dlb
        return jnp.concatenate([dvb, dlb], axis=1)

    def ahead(u, carry):
        acc = jnp.zeros((tokens, hv), F32)
        for k in range(nz):
            acc = acc + dot(gs[2, u, :, cols(k)], w_back(1, k))
        both = adapter_side(1, u, acc)
        for k in range(nz):
            pre[u, :, cols(k)] = dot_nt(both, w_in(1, k))
        return carry

    @pl.when(x == nx - 1)
    def _():
        lax.fori_loop(0, 3, ahead, 0)

    def input_grad(l, u, both, product, after):
        mean = jnp.sum(both.astype(F32) * raw[l, u], axis=-1, keepdims=True) * (1.0 / d_all)
        inv = iv[l, u][:, :1]
        scale = inv * inv * mean
        for p in range(PIECES):
            for k in range(p * per_piece, (p + 1) * per_piece):
                g = product(k) - xs[l, u, :, cols(k)].astype(F32) * scale
                gs[l, u, :, cols(k)] = (gs[l + 1, u, :, cols(k)].astype(F32) + inv * g).astype(BF16)
            after(p)

    def hand_out(l, u):
        @pl.when(yh == l)
        def _():
            pltpu.make_async_copy(gs.at[l, u], out.at[3 * yh + u], os.at[0, u]).start()

        @pl.when(yh != l)
        def _():
            send(gs.at[l, u], out.at[3 * yh + u], os.at[1, u], os.at[2, u], d_yo)

    def run_backward(u):
        @pl.when(x == nx - 1)
        def _():
            both = jnp.concatenate([dv[1, u], dl[1, u]], axis=1)
            input_grad(1, u, both, lambda k: pre[u, :, cols(k)], lambda p: None)

        @pl.when(x < nx - 1)
        def _():
            acc = jnp.zeros((tokens, hv), F32)
            for p in range(PIECES):
                got(piece(gs, 2, u, p), br.at[u, p])
                for k in range(p * per_piece, (p + 1) * per_piece):
                    acc = acc + dot(gs[2, u, :, cols(k)], w_back(1, k))
            both = adapter_side(1, u, acc)
            input_grad(1, u, both, lambda k: dot_nt(both, w_in(1, k)), lambda p: None)

        hand_out(1, u)
        acc = jnp.zeros((tokens, hv), F32)
        for k in range(nz):
            acc = acc + dot(gs[1, u, :, cols(k)], w_back(0, k))
        both = adapter_side(0, u, acc)

        def after(p):
            for q in (p - 1,) if p < PIECES - 1 else (p - 1, p):
                if q >= 0:

                    @pl.when(x > 0)
                    def _(q=q):
                        send(piece(gs, 0, u, q), piece(gs, 2, u, q), bs.at[u, q], br.at[u, q], d_xm)

        input_grad(0, u, both, lambda k: dot_nt(both, w_in(0, k)), after)
        hand_out(0, u)

    pad = jnp.zeros((128 - 3 * tokens, 128), BF16)

    def turn_normed():
        def layer(l, carry):
            inv = iv[l].reshape(3 * tokens, 128)[:, :1]
            for k in range(2 * nz):
                lane = pl.ds(128 * k, 128)
                n_k = xs[l, :, :, lane].reshape(3 * tokens, 128).astype(F32) * inv
                nt[l, lane, :] = jnp.concatenate([n_k.astype(BF16), pad], axis=0).T
            return carry

        lax.fori_loop(0, 2, layer, 0)

    last = x // (nx - 1)

    def turn(t, carry):
        u = last * ((t // 2) % 3) + (1 - last) * (t % 4)
        kind = last * (t % 2 + 2 * (t // 6)) + (1 - last) * (t // 4 + 2 * ((t % 4) // 3))

        @pl.when(kind == 0)
        def _():
            run_forward(u)

        @pl.when(kind == 1)
        def _():
            run_backward(u)

        @pl.when(kind == 2)
        def _():
            turn_normed()

        return carry

    lax.fori_loop(0, 7, turn, 0)

    def adapter_grads(l, carry):
        dl_all = jnp.concatenate([dl[l].reshape(3 * tokens, 128), pad], axis=0)
        lo_all = lo[l].reshape(3 * tokens, 128)
        for k in range(nz):
            g = dot(nt[l, cols(k), :], dl_all).astype(BF16)
            for q in range(4):
                rr[2 * l + q // 2, k, q % 2, pl.ds(0, 64), :] = g[64 * q : 64 * q + 64]
        dv_all = dv[l].reshape(3 * tokens, hv)
        g = lax.dot_general(dv_all, lo_all, TN, preferred_element_type=F32).reshape(nz, 4, 8, 128)
        for q in range(4):
            g_q = g[:, q]
            padded = jnp.concatenate([g_q, jnp.zeros_like(g_q)], axis=1).astype(BF16)
            rr[2 * l + q // 2, :, q % 2, pl.ds(64, 16), :] = padded
        return carry

    lax.fori_loop(0, 2, adapter_grads, 0)

    halves = ((0, 48), (48, 32))
    lo_z, hi_z = pl.ds(0, nh), pl.ds(nh, nh)

    def rows_of(h):
        return pl.ds(*halves[h])

    for h in range(2):
        r = rows_of(h)
        send(rr.at[:, :, 1 - c, r, :], rc.at[:, :, r, :], gsm.at[h, 0], gsm.at[h, 1], d_sib)
    for h in range(2):
        r = rows_of(h)
        got(rc.at[:, :, r, :], gsm.at[h, 1])

        def add_core(i, carry, r=r):
            s1[i, :, r, :] = (rr[i, :, c, r, :].astype(F32) + rc[i, :, r, :].astype(F32)).astype(BF16)
            return carry

        lax.fori_loop(0, NY, add_core, 0)
        send(s1.at[yo, lo_z, r, :], t1.at[:, r, :], gsm.at[h, 2], gsm.at[h, 3], d_yp)
        send(s1.at[yo, hi_z, r, :], t2.at[:, r, :], gsm.at[h, 4], gsm.at[h, 5], d_ym)
    for h in range(2):
        r = rows_of(h)
        got(t1.at[:, r, :], gsm.at[h, 3])
        s1[yp, lo_z, r, :] = (s1[yp, lo_z, r, :].astype(F32) + t1[:, r, :].astype(F32)).astype(BF16)
        got(t2.at[:, r, :], gsm.at[h, 5])
        s1[ym, hi_z, r, :] = (s1[ym, hi_z, r, :].astype(F32) + t2[:, r, :].astype(F32)).astype(BF16)
        send(s1.at[yp, :, r, :], v1.at[:, r, :], gsm.at[h, 6], gsm.at[h, 7], d_yp)
        send(s1.at[ym, :, r, :], v2.at[:, r, :], gsm.at[h, 8], gsm.at[h, 9], d_ym)
    for h in range(2):
        r = rows_of(h)
        got(v1.at[:, r, :], gsm.at[h, 7])
        got(v2.at[:, r, :], gsm.at[h, 9])
        total = s1[y, :, r, :].astype(F32) + v1[:, r, :].astype(F32) + v2[:, r, :].astype(F32)
        s2[:, r, :] = total.astype(BF16)

        def z_send(i, carry, h=h, r=r):
            zz = (z + i) % nz
            send(s2.at[zz, r, :], zb.at[i, r, :], gsm.at[h, 10], zrr.at[h, i], dev(x, y, zz, c))
            return carry

        lax.fori_loop(1, nz, z_send, 0)

    def z_sum(h):
        r = rows_of(h)

        def z_add(i, acc):
            got(zb.at[i, r, :], zrr.at[h, i])
            return acc + zb[i, r, :].astype(F32)

        return lax.fori_loop(1, nz, z_add, s2[z, r, :].astype(F32))

    top, bottom = z_sum(0), z_sum(1)
    gdown[pl.ds(0, 48)] = top
    gdown[pl.ds(48, 16)] = bottom[:16]
    gup[...] = bottom[16:24]

    for h in range(2):
        r = rows_of(h)
        left(zb.at[pl.ds(0, nz - 1), r, :], gsm.at[h, 10])
        left(rc.at[:, :, r, :], gsm.at[h, 0])
        left(t1.at[:, r, :], gsm.at[h, 2])
        left(t2.at[:, r, :], gsm.at[h, 4])
        left(v1.at[:, r, :], gsm.at[h, 6])
        left(v2.at[:, r, :], gsm.at[h, 8])
    for u in range(3):
        for p in range(PIECES):

            @pl.when(x < nx - 1)
            def _(u=u, p=p):
                left(piece(xs, 2, u, p), fs.at[u, p])

            @pl.when(x > 0)
            def _(u=u, p=p):
                left(piece(gs, 0, u, p), bs.at[u, p])

        pltpu.make_async_copy(gs.at[0, u], out.at[3 * yh + u], os.at[0, u]).wait()
        left(gs.at[0, u], os.at[1, u])
        got(out.at[3 * (1 - yh) + u], os.at[2, u])


def run_all(dm, order, wv, wo, ad, au, tok, cot):
    nz, d, hv, t = dm.nz, dm.d, dm.hv, dm.rows
    vm = pltpu.VMEM
    dma = pltpu.SemaphoreType.DMA
    in_vmem = pl.BlockSpec(memory_space=vm)
    anywhere = pl.BlockSpec(memory_space=pl.ANY)
    return pl.pallas_call(
        functools.partial(kernel, dm),
        out_shape=(
            jax.ShapeDtypeStruct((6, t, d), BF16),
            jax.ShapeDtypeStruct((64, 128), F32),
            jax.ShapeDtypeStruct((8, 128), F32),
        ),
        in_specs=[pl.BlockSpec(memory_space=pltpu.SMEM)] + [in_vmem] * 4 + [anywhere] * 2,
        out_specs=(anywhere, in_vmem, in_vmem),
        scratch_shapes=[
            vm((dm.shard, 128), BF16),
            vm((6, t, d), BF16),
            vm((8 * nz, dm.shard, 128), BF16),
            vm((3, 3, t, d), BF16),
            vm((2, d, 128), BF16),
            vm((2, 3, t, 128), F32),
            vm((2, 3, t, hv + 128), F32),
            vm((3, t, d), F32),
            vm((2, 3, t, 128), BF16),
            vm((3, 3, t, d), BF16),
            vm((2, 3, t, hv), BF16),
            vm((2, 3, t, 128), BF16),
            vm((2, hv, 128), BF16),
            vm((4, nz, 2, 80, 128), BF16),
            vm((4, nz, 80, 128), BF16),
            vm((4, nz, 80, 128), BF16),
            vm((dm.nh, 80, 128), BF16),
            vm((dm.nh, 80, 128), BF16),
            vm((nz, 80, 128), BF16),
            vm((nz, 80, 128), BF16),
            vm((nz, 80, 128), BF16),
            vm((nz, 80, 128), BF16),
            dma((2, dm.nh + 2, 4)),
            dma((nz, 4)),
            dma((12,)),
            dma((4,)),
            dma((3, PIECES)),
            dma((3, PIECES)),
            dma((3, PIECES)),
            dma((3, PIECES)),
            dma((3, 3)),
            dma((2, 11)),
            dma((2, nz)),
        ],
        compiler_params=pltpu.CompilerParams(
            collective_id=0, has_side_effects=True, vmem_limit_bytes=44 * 1024 * 1024
        ),
        name="relay",
    )(order, wv, wo, ad, au, tok, cot)


def solution(mesh):
    def body(tokens, cotangent, order, w_value, w_out, adapter_down, adapter_up):
        dm = Dims(mesh, tokens.shape[1], tokens.shape[2], w_value.shape[2])
        dx, down, up = run_all(
            dm, order, w_value[0], w_out[0].T, adapter_down[0], adapter_up[0].T, tokens, cotangent
        )
        return (dx[None], down[None], up.T[None])

    return jax.shard_map(
        body,
        mesh=mesh,
        in_specs=(
            P(None, "fsdp", None),
            P(None, "fsdp", None),
            P(),
            P("section", "fsdp", None),
            P("section", None, "fsdp"),
            P("section", "fsdp", None),
            P("section", None, "fsdp"),
        ),
        out_specs=(
            P("section", None, "fsdp", None),
            P("section", "fsdp", None),
            P("section", None, "fsdp"),
        ),
        check_vma=False,
    )
```

```python
import functools

import jax
import jax.numpy as jnp
from jax import lax
from jax.experimental import pallas as pl
from jax.experimental.pallas import tpu as pltpu
from jax.sharding import PartitionSpec as P

EPS = 1e-05
MESH = pl.DeviceIdType.MESH
F32 = jnp.float32
BF16 = jnp.bfloat16
NT = (((1,), (1,)), ((), ()))
TN = (((0,), (0,)), ((), ()))
NY = 4
PIECES = 4


def dot(a, b):
    return jnp.dot(a, b, preferred_element_type=F32)


def dot_nt(a, b):
    return lax.dot_general(a, b, NT, preferred_element_type=F32)


class Dims:
    def __init__(self, mesh, rows, width, hv):
        self.nx = mesh.shape["section"] // 2
        self.nz = mesh.shape["fsdp"] // 4
        self.nh = self.nz // 2
        self.rows = rows
        self.d = width
        self.hv = hv
        self.hb = hv // 128
        self.off_out = 64 * self.hb
        self.off_down = 128 * self.hb
        self.off_up = self.off_down + 64
        self.shard = self.off_up + 16
        tiles = self.shard // 16
        self.rp = (tiles * 351 // 1000 + 1) * 16 if tiles < 37 else 208
        self.half = max((tiles + 1) // 2 * 16, self.rp)
        self.qa = self.rp + (tiles - self.rp // 16) // 2 * 16


def kernel(dm, order, wv_in, wo_in, ad_in, au_in, tok, cot, out, gdown, gup, wv, wo, ad, au, shard, stage, buf, xs, nt, iv, raw, pre, lo, gs, dv, dl,
           up, rr, rc, s1, t1, t2, v1, v2, s2, zb, ins, zr, yr, ss, cs, fr, fs, br, bs, os, gsm, zrr):
    nx, nz, nh, d_all, hv, hb = dm.nx, dm.nz, dm.nh, dm.d, dm.hv, dm.hb
    sec = lax.axis_index("section")
    fid = lax.axis_index("fsdp")
    x = sec // 2
    yh = sec % 2
    z = fid // 4
    y = yh * 2 + (fid // 2) % 2
    c = fid % 2
    yp, ym, yo = (y + 1) % NY, (y + NY - 1) % NY, (y + 2) % NY
    zp, zm = (z + 1) % nz, (z + nz - 1) % nz

    def dev(x_, y_, z_, c_):
        return (x_ * 2 + y_ // 2, z_ * 4 + (y_ % 2) * 2 + c_)

    def slot(y_, z_, c_):
        return (y_ // 2) * (4 * nz) + z_ * 4 + (y_ % 2) * 2 + c_

    d_zp, d_zm = dev(x, y, zp, c), dev(x, y, zm, c)
    d_yp, d_ym, d_yo = dev(x, yp, z, c), dev(x, ym, z, c), dev(x, yo, z, c)
    d_sib = dev(x, y, z, 1 - c)
    d_xp, d_xm = dev(x + 1, y, z, c), dev(x - 1, y, z, c)

    def send(src, dst, ssem, rsem, to):
        pltpu.make_async_remote_copy(
            src_ref=src, dst_ref=dst, send_sem=ssem, recv_sem=rsem, device_id=to, device_id_type=MESH
        ).start()

    def got(ref, rsem):
        pltpu.make_async_remote_copy(
            src_ref=ref, dst_ref=ref, send_sem=rsem, recv_sem=rsem, device_id=d_sib, device_id_type=MESH
        ).wait_recv()

    def left(ref, ssem):
        pltpu.make_async_remote_copy(
            src_ref=ref, dst_ref=ref, send_sem=ssem, recv_sem=ssem, device_id=d_sib, device_id_type=MESH
        ).wait_send()

    barrier = pltpu.get_barrier_semaphore()

    def greet(to):
        pl.semaphore_signal(barrier, inc=1, device_id=to, device_id_type=MESH)

    d_xs = dev((x + nx - 1) % nx, y, z, c), dev((x + 1) % nx, y, z, c)
    peers = (d_sib, d_yp, d_ym, d_zp, d_zm, *d_xs)
    for to in peers:
        greet(to)
    fetches = [
        pltpu.make_async_copy(src, dst, ins.at[i])
        for i, (src, dst) in enumerate(((wv_in, wv), (wo_in, wo), (ad_in, ad), (au_in, au)))
    ]
    for f in fetches:
        f.start()

    @pl.when(x == 0)
    def _():
        pltpu.make_async_copy(tok, stage, cs.at[3]).start()

    @pl.when(x == nx - 1)
    def _():
        pltpu.make_async_copy(cot, stage, cs.at[3]).start()

    for f in fetches:
        f.wait()
    for b in range(hb):
        shard[pl.ds(64 * b, 64)] = wv[:, 128 * b : 128 * b + 128]
        shard[pl.ds(dm.off_out + 64 * b, 64)] = wo[:, 128 * b : 128 * b + 128]
    shard[pl.ds(dm.off_down, 64)] = ad[...]
    turned = au[...].astype(F32)
    shard[pl.ds(dm.off_up, 16)] = jnp.concatenate([turned, jnp.zeros_like(turned)], axis=0).astype(BF16)

    pl.semaphore_wait(barrier, len(peers))

    rows, rp, half, qa = dm.shard, dm.rp, dm.half, dm.qa

    def part(s, r0, r1):
        return buf.at[s, pl.ds(r0, r1 - r0), :]

    def to_sib(s, r0, r1):
        send(part(s, r0, r1), part(s, r0, r1), cs.at[0], cs.at[1], d_sib)

    def move(s, r0, r1, ssem, rsem, to):
        send(part(s, r0, r1), part(s, r0, r1), ssem, rsem, to)

    me = slot(y, z, c)
    own = buf.at[me]
    send(shard, own, ss.at[0], zr.at[0, 1, 0], d_zp)
    send(shard, own, ss.at[1], zr.at[1, 1, 0], d_zm)
    send(shard, own, ss.at[4], yr.at[0, 0], d_yp)
    send(shard, own, ss.at[11], yr.at[0, 1], d_ym)
    send(shard, own, cs.at[0], cs.at[1], d_sib)
    local = pltpu.make_async_copy(shard, own, cs.at[2])
    local.start()

    @pl.when(x == 0)
    def _():
        pltpu.make_async_copy(tok, stage, cs.at[3]).wait()
        for u in range(3):
            xs[0, u] = stage[order[3 * yh + u]]

    @pl.when(x == nx - 1)
    def _():
        pltpu.make_async_copy(cot, stage, cs.at[3]).wait()
        for u in range(3):
            gs[2, u] = stage[order[3 * yh + u]]

    def send_p(s, kind, dist_of):
        for way, (ps, to) in enumerate(((2, d_zp), (3, d_zm))):
            move(s, 0, rp, ss.at[ps], zr.at[way, dist_of, kind], to)

    s_m, s_p, s_o = slot(ym, z, c), slot(yp, z, c), slot(yo, z, c)
    got(part(s_m, 0, rows), yr.at[0, 0])
    move(s_m, 0, half, ss.at[5], yr.at[0, 2], d_yp)
    send_p(s_m, 2, 1)
    to_sib(s_m, 0, rows)
    got(part(s_p, 0, rows), yr.at[0, 1])
    move(s_p, half, rows, ss.at[6], yr.at[0, 3], d_ym)
    send_p(s_p, 1, 1)
    to_sib(s_p, 0, rows)

    def z_from(way, d):
        return (z + nz - d) % nz if way == 0 else (z + d) % nz

    def e_of(way, d):
        return d if way == 0 else nh + d

    def limit(way):
        return nh if way == 0 else nh - 1

    def limit_p(way):
        return nh - 1 if way == 0 else nh

    def z_shard(way, d):
        s = slot(y, z_from(way, d), c)
        e = e_of(way, d)
        got(part(s, 0, rows), zr.at[way, d, 0])

        @pl.when(d < limit(way))
        def _():
            move(s, 0, rows, ss.at[way], zr.at[way, d + 1, 0], (d_zp, d_zm)[way])

        move(s, rp, rows, ss.at[7], yr.at[e, 0], d_yp)
        move(s, rp, rows, ss.at[8], yr.at[e, 1], d_ym)
        to_sib(s, 0, rows)

    def z_parts(way, d):
        for kind, col in ((2, ym), (1, yp), (3, yo)):
            s = slot(col, z_from(way, d), c)
            got(part(s, 0, rp), zr.at[way, d, kind])

            @pl.when(d < limit_p(way))
            def _(s=s, kind=kind):
                move(s, 0, rp, ss.at[2 + way], zr.at[way, d + 1, kind], (d_zp, d_zm)[way])

            to_sib(s, 0, rp)

    def y_near(way, d):
        e, zz = e_of(way, d), z_from(way, d)
        a, b = slot(ym, zz, c), slot(yp, zz, c)
        got(part(a, rp, rows), yr.at[e, 0])
        move(a, rp, qa, ss.at[9], yr.at[e, 2], d_yp)
        to_sib(a, rp, rows)
        got(part(b, rp, rows), yr.at[e, 1])
        move(b, qa, rows, ss.at[10], yr.at[e, 3], d_ym)
        to_sib(b, rp, rows)

    def y_far(way, d):
        e, zz = e_of(way, d), z_from(way, d)
        s = slot(yo, zz, c)
        got(part(s, rp, qa), yr.at[e, 2])
        to_sib(s, rp, qa)
        got(part(s, qa, rows), yr.at[e, 3])
        to_sib(s, qa, rows)

    def gather_step(d, carry):
        for way in (0, 1):
            pl.when(d <= limit(way))(functools.partial(z_shard, way, d))

        @pl.when(d == 1)
        def _():
            got(part(s_o, 0, half), yr.at[0, 2])
            send_p(s_o, 3, 1)
            to_sib(s_o, 0, half)
            got(part(s_o, half, rows), yr.at[0, 3])
            to_sib(s_o, half, rows)

        for way in (0, 1):
            pl.when(d <= limit_p(way))(functools.partial(z_parts, way, d))
        for way in (0, 1):
            pl.when((d > 1) & (d <= limit(way) + 1))(functools.partial(y_near, way, d - 1))
        for way in (0, 1):
            pl.when((d > 2) & (d <= limit(way) + 2))(functools.partial(y_far, way, d - 2))
        return carry

    lax.fori_loop(1, nh + 3, gather_step, 0)

    local.wait()
    half_all = buf.at[pl.ds(0, 4 * nz)]
    got(half_all, cs.at[1])

    for l in range(2):
        packed = buf[pl.ds(l * 4 * nz, 4 * nz), pl.ds(dm.off_up, 16), :].astype(F32)
        up[l] = packed[:, :8, :].reshape(hv, 128).astype(BF16)

    tokens = dm.rows

    def block(l, k, off):
        return buf[pl.ds(l * 4 * nz + 4 * k, 4), pl.ds(off, 64), :].reshape(256, 128)

    def w_in(l, k):
        return jnp.concatenate([block(l, k, 64 * b) for b in range(hb)] + [block(l, k, dm.off_down)], axis=1)

    def w_back(l, k):
        return jnp.concatenate([block(l, k, dm.off_out + 64 * b) for b in range(hb)], axis=1)

    def cols(k):
        return pl.ds(256 * k, 256)

    width = d_all // PIECES
    per_piece = nz // PIECES

    def piece(ref, i, u, p):
        return ref.at[i, u, :, pl.ds(width * p, width)]

    def lanes(v):
        return v[:, :128] + v[:, 128:]

    def run_forward(u):
        for l in range(2):
            total = jnp.zeros((tokens, 128), F32)
            acc = jnp.zeros((tokens, hv + 128), F32)
            for p in range(PIECES):
                if l == 0:

                    @pl.when(x > 0)
                    def _(p=p):
                        got(piece(xs, 0, u, p), fr.at[u, p])

                for k in range(p * per_piece, (p + 1) * per_piece):
                    v = xs[l, u, :, cols(k)]
                    acc = acc + dot(v, w_in(l, k))
                    v = v.astype(F32)
                    total = total + lanes(v * v)
            inv = lax.rsqrt(jnp.sum(total, axis=-1, keepdims=True) * (1.0 / d_all) + EPS)
            iv[l, u] = jnp.broadcast_to(inv, (tokens, 128))
            raw[l, u] = acc
            acc = acc * inv
            low = acc[:, hv:].astype(BF16)
            lo[l, u] = low
            val = (acc[:, :hv] + dot_nt(low, up[l])).astype(BF16)

            def outputs(l=l, val=val):
                for p in range(PIECES):
                    for k in range(p * per_piece, (p + 1) * per_piece):
                        o = xs[l, u, :, cols(k)].astype(F32) + dot_nt(val, w_back(l, k))
                        xs[l + 1, u, :, cols(k)] = o.astype(BF16)
                    if l == 1:
                        for q in (p - 1,) if p < PIECES - 1 else (p - 1, p):
                            if q >= 0:
                                send(piece(xs, 2, u, q), piece(xs, 0, u, q), fs.at[u, q], fr.at[u, q], d_xp)

            if l == 0:
                outputs()
            else:
                pl.when(x < nx - 1)(outputs)

    def adapter_side(l, u, acc):
        dvb = acc.astype(BF16)
        dv[l, u] = dvb
        dlb = dot(dvb, up[l]).astype(BF16)
        dl[l, u] = dlb
        return jnp.concatenate([dvb, dlb], axis=1)

    def ahead(u, carry):
        acc = jnp.zeros((tokens, hv), F32)
        for k in range(nz):
            acc = acc + dot(gs[2, u, :, cols(k)], w_back(1, k))
        both = adapter_side(1, u, acc)
        for k in range(nz):
            pre[u, :, cols(k)] = dot_nt(both, w_in(1, k))
        return carry

    @pl.when(x == nx - 1)
    def _():
        lax.fori_loop(0, 3, ahead, 0)

    def input_grad(l, u, both, product, after):
        mean = jnp.sum(both.astype(F32) * raw[l, u], axis=-1, keepdims=True) * (1.0 / d_all)
        inv = iv[l, u][:, :1]
        scale = inv * inv * mean
        for p in range(PIECES):
            for k in range(p * per_piece, (p + 1) * per_piece):
                g = product(k) - xs[l, u, :, cols(k)].astype(F32) * scale
                gs[l, u, :, cols(k)] = (gs[l + 1, u, :, cols(k)].astype(F32) + inv * g).astype(BF16)
            after(p)

    def hand_out(l, u):
        @pl.when(yh == l)
        def _():
            pltpu.make_async_copy(gs.at[l, u], out.at[3 * yh + u], os.at[0, u]).start()

        @pl.when(yh != l)
        def _():
            send(gs.at[l, u], out.at[3 * yh + u], os.at[1, u], os.at[2, u], d_yo)

    def run_backward(u):
        @pl.when(x == nx - 1)
        def _():
            both = jnp.concatenate([dv[1, u], dl[1, u]], axis=1)
            input_grad(1, u, both, lambda k: pre[u, :, cols(k)], lambda p: None)

        @pl.when(x < nx - 1)
        def _():
            acc = jnp.zeros((tokens, hv), F32)
            for p in range(PIECES):
                got(piece(gs, 2, u, p), br.at[u, p])
                for k in range(p * per_piece, (p + 1) * per_piece):
                    acc = acc + dot(gs[2, u, :, cols(k)], w_back(1, k))
            both = adapter_side(1, u, acc)
            input_grad(1, u, both, lambda k: dot_nt(both, w_in(1, k)), lambda p: None)

        hand_out(1, u)
        acc = jnp.zeros((tokens, hv), F32)
        for k in range(nz):
            acc = acc + dot(gs[1, u, :, cols(k)], w_back(0, k))
        both = adapter_side(0, u, acc)

        def after(p):
            for q in (p - 1,) if p < PIECES - 1 else (p - 1, p):
                if q >= 0:

                    @pl.when(x > 0)
                    def _(q=q):
                        send(piece(gs, 0, u, q), piece(gs, 2, u, q), bs.at[u, q], br.at[u, q], d_xm)

        input_grad(0, u, both, lambda k: dot_nt(both, w_in(0, k)), after)
        hand_out(0, u)

    pad = jnp.zeros((128 - 3 * tokens, 128), BF16)

    def turn_normed():
        def layer(l, carry):
            inv = iv[l].reshape(3 * tokens, 128)[:, :1]
            for k in range(2 * nz):
                lane = pl.ds(128 * k, 128)
                n_k = xs[l, :, :, lane].reshape(3 * tokens, 128).astype(F32) * inv
                nt[l, lane, :] = jnp.concatenate([n_k.astype(BF16), pad], axis=0).T
            return carry

        lax.fori_loop(0, 2, layer, 0)

    last = x // (nx - 1)

    def turn(t, carry):
        u = last * ((t // 2) % 3) + (1 - last) * (t % 4)
        kind = last * (t % 2 + 2 * (t // 6)) + (1 - last) * (t // 4 + 2 * ((t % 4) // 3))

        @pl.when(kind == 0)
        def _():
            run_forward(u)

        @pl.when(kind == 1)
        def _():
            run_backward(u)

        @pl.when(kind == 2)
        def _():
            turn_normed()

        return carry

    lax.fori_loop(0, 7, turn, 0)

    def adapter_grads(l):
        dl_all = jnp.concatenate([dl[l].reshape(3 * tokens, 128), pad], axis=0)
        lo_all = lo[l].reshape(3 * tokens, 128)
        for k in range(nz):
            g = dot(nt[l, cols(k), :], dl_all).astype(BF16)
            for q in range(4):
                rr[2 * l + q // 2, k, q % 2, pl.ds(0, 64), :] = g[64 * q : 64 * q + 64]
        dv_all = dv[l].reshape(3 * tokens, hv)
        g = lax.dot_general(dv_all, lo_all, TN, preferred_element_type=F32).reshape(nz, 4, 8, 128)
        for q in range(4):
            g_q = g[:, q]
            padded = jnp.concatenate([g_q, jnp.zeros_like(g_q)], axis=1).astype(BF16)
            rr[2 * l + q // 2, :, q % 2, pl.ds(64, 16), :] = padded

    for l in range(2):
        adapter_grads(l)
        two = pl.ds(2 * l, 2)
        send(rr.at[two, :, 1 - c], rc.at[two], gsm.at[l, 0], gsm.at[l, 1], d_sib)

    halves = ((0, 48), (48, 32))
    lo_z, hi_z = pl.ds(0, nh), pl.ds(nh, nh)

    def rows_of(h):
        return pl.ds(*halves[h])

    for l in range(2):
        got(rc.at[pl.ds(2 * l, 2)], gsm.at[l, 1])
    for h in range(2):
        r = rows_of(h)

        def add_core(i, carry, r=r):
            s1[i, :, r, :] = (rr[i, :, c, r, :].astype(F32) + rc[i, :, r, :].astype(F32)).astype(BF16)
            return carry

        lax.fori_loop(0, NY, add_core, 0)
        send(s1.at[yo, lo_z, r, :], t1.at[:, r, :], gsm.at[h, 2], gsm.at[h, 3], d_yp)
        send(s1.at[yo, hi_z, r, :], t2.at[:, r, :], gsm.at[h, 4], gsm.at[h, 5], d_ym)
    for h in range(2):
        r = rows_of(h)
        got(t1.at[:, r, :], gsm.at[h, 3])
        s1[yp, lo_z, r, :] = (s1[yp, lo_z, r, :].astype(F32) + t1[:, r, :].astype(F32)).astype(BF16)
        got(t2.at[:, r, :], gsm.at[h, 5])
        s1[ym, hi_z, r, :] = (s1[ym, hi_z, r, :].astype(F32) + t2[:, r, :].astype(F32)).astype(BF16)
        send(s1.at[yp, :, r, :], v1.at[:, r, :], gsm.at[h, 6], gsm.at[h, 7], d_yp)
        send(s1.at[ym, :, r, :], v2.at[:, r, :], gsm.at[h, 8], gsm.at[h, 9], d_ym)
    for h in range(2):
        r = rows_of(h)
        got(v1.at[:, r, :], gsm.at[h, 7])
        got(v2.at[:, r, :], gsm.at[h, 9])
        total = s1[y, :, r, :].astype(F32) + v1[:, r, :].astype(F32) + v2[:, r, :].astype(F32)
        s2[:, r, :] = total.astype(BF16)

        def z_send(j, carry, h=h, r=r):
            def to(i):
                zz = (z + i) % nz
                send(s2.at[zz, r, :], zb.at[i, r, :], gsm.at[h, 10], zrr.at[h, i], dev(x, y, zz, c))

            to(nh - j)

            @pl.when(j > 0)
            def _():
                to(nh + j)

            return carry

        lax.fori_loop(0, nh, z_send, 0)

    def z_sum(h):
        r = rows_of(h)

        def z_add(i, acc):
            got(zb.at[i, r, :], zrr.at[h, i])
            return acc + zb[i, r, :].astype(F32)

        return lax.fori_loop(1, nz, z_add, s2[z, r, :].astype(F32))

    top, bottom = z_sum(0), z_sum(1)
    gdown[pl.ds(0, 48)] = top
    gdown[pl.ds(48, 16)] = bottom[:16]
    gup[...] = bottom[16:24]

    left(half_all, cs.at[0])

    def span(n, r):
        return buf.at[pl.ds(0, n), pl.ds(0, r), :]

    left(span(nh, rows), ss.at[0])
    left(span(nh - 1, rows), ss.at[1])
    left(span(3 * (nh - 1), rp), ss.at[2])
    left(span(3 * nh, rp), ss.at[3])
    left(span(1, rows), ss.at[4])
    left(span(1, rows), ss.at[11])
    left(span(1, half), ss.at[5])
    left(span(1, rows - half), ss.at[6])
    left(span(nz - 1, rows - rp), ss.at[7])
    left(span(nz - 1, rows - rp), ss.at[8])
    left(span(nz - 1, qa - rp), ss.at[9])
    left(span(nz - 1, rows - qa), ss.at[10])
    for h in range(2):
        r = rows_of(h)
        left(zb.at[pl.ds(0, nz - 1), r, :], gsm.at[h, 10])
        left(rc.at[pl.ds(2 * h, 2)], gsm.at[h, 0])
        left(t1.at[:, r, :], gsm.at[h, 2])
        left(t2.at[:, r, :], gsm.at[h, 4])
        left(v1.at[:, r, :], gsm.at[h, 6])
        left(v2.at[:, r, :], gsm.at[h, 8])
    for u in range(3):
        for p in range(PIECES):

            @pl.when(x < nx - 1)
            def _(u=u, p=p):
                left(piece(xs, 2, u, p), fs.at[u, p])

            @pl.when(x > 0)
            def _(u=u, p=p):
                left(piece(gs, 0, u, p), bs.at[u, p])

        pltpu.make_async_copy(gs.at[0, u], out.at[3 * yh + u], os.at[0, u]).wait()
        left(gs.at[0, u], os.at[1, u])
        got(out.at[3 * (1 - yh) + u], os.at[2, u])


def run_all(dm, order, wv, wo, ad, au, tok, cot):
    nz, d, hv, t = dm.nz, dm.d, dm.hv, dm.rows
    vm = pltpu.VMEM
    dma = pltpu.SemaphoreType.DMA
    in_vmem = pl.BlockSpec(memory_space=vm)
    anywhere = pl.BlockSpec(memory_space=pl.ANY)
    in_hbm = pl.BlockSpec(memory_space=pltpu.HBM)
    return pl.pallas_call(
        functools.partial(kernel, dm),
        out_shape=(
            jax.ShapeDtypeStruct((6, t, d), BF16),
            jax.ShapeDtypeStruct((64, 128), F32),
            jax.ShapeDtypeStruct((8, 128), F32),
        ),
        in_specs=[pl.BlockSpec(memory_space=pltpu.SMEM)] + [in_hbm] * 6,
        out_specs=(anywhere, in_vmem, in_vmem),
        scratch_shapes=[
            *(vm(a.shape, BF16) for a in (wv, wo, ad, au)),
            vm((dm.shard, 128), BF16),
            vm((6, t, d), BF16),
            vm((8 * nz, dm.shard, 128), BF16),
            vm((3, 3, t, d), BF16),
            vm((2, d, 128), BF16),
            vm((2, 3, t, 128), F32),
            vm((2, 3, t, hv + 128), F32),
            vm((3, t, d), F32),
            vm((2, 3, t, 128), BF16),
            vm((3, 3, t, d), BF16),
            vm((2, 3, t, hv), BF16),
            vm((2, 3, t, 128), BF16),
            vm((2, hv, 128), BF16),
            vm((4, nz, 2, 80, 128), BF16),
            vm((4, nz, 80, 128), BF16),
            vm((4, nz, 80, 128), BF16),
            vm((dm.nh, 80, 128), BF16),
            vm((dm.nh, 80, 128), BF16),
            vm((nz, 80, 128), BF16),
            vm((nz, 80, 128), BF16),
            vm((nz, 80, 128), BF16),
            vm((nz, 80, 128), BF16),
            dma((4,)),
            dma((2, dm.nh + 2, 4)),
            dma((nz, 4)),
            dma((12,)),
            dma((4,)),
            dma((3, PIECES)),
            dma((3, PIECES)),
            dma((3, PIECES)),
            dma((3, PIECES)),
            dma((3, 3)),
            dma((2, 11)),
            dma((2, nz)),
        ],
        compiler_params=pltpu.CompilerParams(
            collective_id=0, has_side_effects=True, vmem_limit_bytes=62 * 1024 * 1024
        ),
        name="relay",
    )(order, wv, wo, ad, au, tok, cot)


def solution(mesh):
    def body(tokens, cotangent, order, w_value, w_out, adapter_down, adapter_up):
        dm = Dims(mesh, tokens.shape[1], tokens.shape[2], w_value.shape[2])
        dx, down, up = run_all(
            dm, order, w_value[0], w_out[0].T, adapter_down[0], adapter_up[0].T, tokens, cotangent
        )
        return (dx[None], down[None], up.T[None])

    return jax.shard_map(
        body,
        mesh=mesh,
        in_specs=(
            P(None, "fsdp", None),
            P(None, "fsdp", None),
            P(),
            P("section", "fsdp", None),
            P("section", None, "fsdp"),
            P("section", "fsdp", None),
            P("section", None, "fsdp"),
        ),
        out_specs=(
            P("section", None, "fsdp", None),
            P("section", "fsdp", None),
            P("section", None, "fsdp"),
        ),
        check_vma=False,
    )
```

```python
import functools

import jax
import jax.numpy as jnp
from jax import lax
from jax.experimental import pallas as pl
from jax.experimental.pallas import tpu as pltpu
from jax.sharding import PartitionSpec as P

EPS = 1e-05
MESH = pl.DeviceIdType.MESH
F32 = jnp.float32
BF16 = jnp.bfloat16
NT = (((1,), (1,)), ((), ()))
TN = (((0,), (0,)), ((), ()))
NY = 4
PIECES = 4


def dot(a, b):
    return jnp.dot(a, b, preferred_element_type=F32)


def dot_nt(a, b):
    return lax.dot_general(a, b, NT, preferred_element_type=F32)


class Dims:
    def __init__(self, mesh, rows, width, hv):
        self.nx = mesh.shape["section"] // 2
        self.nz = mesh.shape["fsdp"] // 4
        self.nh = self.nz // 2
        self.rows = rows
        self.d = width
        self.hv = hv
        self.hb = hv // 128
        self.off_out = 64 * self.hb
        self.off_down = 128 * self.hb
        self.off_up = self.off_down + 64
        self.shard = self.off_up + 16
        tiles = self.shard // 16
        self.rp = (tiles * 351 // 1000 + 1) * 16 if tiles < 37 else 208
        self.half = max((tiles + 1) // 2 * 16, self.rp)
        self.qa = self.rp + (tiles - self.rp // 16) // 2 * 16


def kernel(dm, order, wv_in, wo_in, ad_in, au_in, tok, cot, out, gdown, gup, wv, wo, ad, au, shard, stage, buf, xs, nt, iv, raw, pre, lo, gs, dv, dl,
           up, rr, rc, s1, t1, t2, v1, v2, s2, zb, zs, zf, ins, zr, yr, ss, cs, fr, fs, br, bs, os, gsm, zrr):
    nx, nz, nh, d_all, hv, hb = dm.nx, dm.nz, dm.nh, dm.d, dm.hv, dm.hb
    sec = lax.axis_index("section")
    fid = lax.axis_index("fsdp")
    x = sec // 2
    yh = sec % 2
    z = fid // 4
    y = yh * 2 + (fid // 2) % 2
    c = fid % 2
    yp, ym, yo = (y + 1) % NY, (y + NY - 1) % NY, (y + 2) % NY
    zp, zm = (z + 1) % nz, (z + nz - 1) % nz

    def dev(x_, y_, z_, c_):
        return (x_ * 2 + y_ // 2, z_ * 4 + (y_ % 2) * 2 + c_)

    def slot(y_, z_, c_):
        return (y_ // 2) * (4 * nz) + z_ * 4 + (y_ % 2) * 2 + c_

    d_zp, d_zm = dev(x, y, zp, c), dev(x, y, zm, c)
    d_yp, d_ym, d_yo = dev(x, yp, z, c), dev(x, ym, z, c), dev(x, yo, z, c)
    d_sib = dev(x, y, z, 1 - c)
    d_xp, d_xm = dev(x + 1, y, z, c), dev(x - 1, y, z, c)

    def send(src, dst, ssem, rsem, to):
        pltpu.make_async_remote_copy(
            src_ref=src, dst_ref=dst, send_sem=ssem, recv_sem=rsem, device_id=to, device_id_type=MESH
        ).start()

    def got(ref, rsem):
        pltpu.make_async_remote_copy(
            src_ref=ref, dst_ref=ref, send_sem=rsem, recv_sem=rsem, device_id=d_sib, device_id_type=MESH
        ).wait_recv()

    def left(ref, ssem):
        pltpu.make_async_remote_copy(
            src_ref=ref, dst_ref=ref, send_sem=ssem, recv_sem=ssem, device_id=d_sib, device_id_type=MESH
        ).wait_send()

    barrier = pltpu.get_barrier_semaphore()

    def greet(to):
        pl.semaphore_signal(barrier, inc=1, device_id=to, device_id_type=MESH)

    d_xs = dev((x + nx - 1) % nx, y, z, c), dev((x + 1) % nx, y, z, c)
    peers = (d_sib, d_yp, d_ym, d_zp, d_zm, *d_xs)
    for to in peers:
        greet(to)
    fetches = [
        pltpu.make_async_copy(src, dst, ins.at[i])
        for i, (src, dst) in enumerate(((wv_in, wv), (wo_in, wo), (ad_in, ad), (au_in, au)))
    ]
    for f in fetches:
        f.start()

    @pl.when(x == 0)
    def _():
        pltpu.make_async_copy(tok, stage, cs.at[3]).start()

    @pl.when(x == nx - 1)
    def _():
        pltpu.make_async_copy(cot, stage, cs.at[3]).start()

    for f in fetches:
        f.wait()
    for b in range(hb):
        shard[pl.ds(64 * b, 64)] = wv[:, 128 * b : 128 * b + 128]
        shard[pl.ds(dm.off_out + 64 * b, 64)] = wo[:, 128 * b : 128 * b + 128]
    shard[pl.ds(dm.off_down, 64)] = ad[...]
    turned = au[...].astype(F32)
    shard[pl.ds(dm.off_up, 16)] = jnp.concatenate([turned, jnp.zeros_like(turned)], axis=0).astype(BF16)

    pl.semaphore_wait(barrier, len(peers))

    rows, rp, half, qa = dm.shard, dm.rp, dm.half, dm.qa

    def part(s, r0, r1):
        return buf.at[s, pl.ds(r0, r1 - r0), :]

    def to_sib(s, r0, r1):
        send(part(s, r0, r1), part(s, r0, r1), cs.at[0], cs.at[1], d_sib)

    def move(s, r0, r1, ssem, rsem, to):
        send(part(s, r0, r1), part(s, r0, r1), ssem, rsem, to)

    me = slot(y, z, c)
    own = buf.at[me]
    send(shard, own, ss.at[0], zr.at[0, 1, 0], d_zp)
    send(shard, own, ss.at[1], zr.at[1, 1, 0], d_zm)
    send(shard, own, ss.at[4], yr.at[0, 0], d_yp)
    send(shard, own, ss.at[11], yr.at[0, 1], d_ym)
    send(shard, own, cs.at[0], cs.at[1], d_sib)
    local = pltpu.make_async_copy(shard, own, cs.at[2])
    local.start()

    @pl.when(x == 0)
    def _():
        pltpu.make_async_copy(tok, stage, cs.at[3]).wait()
        for u in range(3):
            xs[0, u] = stage[order[3 * yh + u]]

    @pl.when(x == nx - 1)
    def _():
        pltpu.make_async_copy(cot, stage, cs.at[3]).wait()
        for u in range(3):
            gs[2, u] = stage[order[3 * yh + u]]

    def send_p(s, kind, dist_of):
        for way, (ps, to) in enumerate(((2, d_zp), (3, d_zm))):
            move(s, 0, rp, ss.at[ps], zr.at[way, dist_of, kind], to)

    s_m, s_p, s_o = slot(ym, z, c), slot(yp, z, c), slot(yo, z, c)
    got(part(s_m, 0, rows), yr.at[0, 0])
    move(s_m, 0, half, ss.at[5], yr.at[0, 2], d_yp)
    send_p(s_m, 2, 1)
    to_sib(s_m, 0, rows)
    got(part(s_p, 0, rows), yr.at[0, 1])
    move(s_p, half, rows, ss.at[6], yr.at[0, 3], d_ym)
    send_p(s_p, 1, 1)
    to_sib(s_p, 0, rows)

    def z_from(way, d):
        return (z + nz - d) % nz if way == 0 else (z + d) % nz

    def e_of(way, d):
        return d if way == 0 else nh + d

    def limit(way):
        return nh if way == 0 else nh - 1

    def limit_p(way):
        return nh - 1 if way == 0 else nh

    def z_shard(way, d):
        s = slot(y, z_from(way, d), c)
        e = e_of(way, d)
        got(part(s, 0, rows), zr.at[way, d, 0])

        @pl.when(d < limit(way))
        def _():
            move(s, 0, rows, ss.at[way], zr.at[way, d + 1, 0], (d_zp, d_zm)[way])

        move(s, rp, rows, ss.at[7], yr.at[e, 0], d_yp)
        move(s, rp, rows, ss.at[8], yr.at[e, 1], d_ym)
        to_sib(s, 0, rows)

    def z_parts(way, d):
        for kind, col in ((2, ym), (1, yp), (3, yo)):
            s = slot(col, z_from(way, d), c)
            got(part(s, 0, rp), zr.at[way, d, kind])

            @pl.when(d < limit_p(way))
            def _(s=s, kind=kind):
                move(s, 0, rp, ss.at[2 + way], zr.at[way, d + 1, kind], (d_zp, d_zm)[way])

            to_sib(s, 0, rp)

    def y_near(way, d):
        e, zz = e_of(way, d), z_from(way, d)
        a, b = slot(ym, zz, c), slot(yp, zz, c)
        got(part(a, rp, rows), yr.at[e, 0])
        move(a, rp, qa, ss.at[9], yr.at[e, 2], d_yp)
        to_sib(a, rp, rows)
        got(part(b, rp, rows), yr.at[e, 1])
        move(b, qa, rows, ss.at[10], yr.at[e, 3], d_ym)
        to_sib(b, rp, rows)

    def y_far(way, d):
        e, zz = e_of(way, d), z_from(way, d)
        s = slot(yo, zz, c)
        got(part(s, rp, qa), yr.at[e, 2])
        to_sib(s, rp, qa)
        got(part(s, qa, rows), yr.at[e, 3])
        to_sib(s, qa, rows)

    def gather_step(d, carry):
        for way in (0, 1):
            pl.when(d <= limit(way))(functools.partial(z_shard, way, d))

        @pl.when(d == 1)
        def _():
            got(part(s_o, 0, half), yr.at[0, 2])
            send_p(s_o, 3, 1)
            to_sib(s_o, 0, half)
            got(part(s_o, half, rows), yr.at[0, 3])
            to_sib(s_o, half, rows)

        for way in (0, 1):
            pl.when(d <= limit_p(way))(functools.partial(z_parts, way, d))
        for way in (0, 1):
            pl.when((d > 1) & (d <= limit(way) + 1))(functools.partial(y_near, way, d - 1))
        for way in (0, 1):
            pl.when((d > 2) & (d <= limit(way) + 2))(functools.partial(y_far, way, d - 2))
        return carry

    lax.fori_loop(1, nh + 3, gather_step, 0)

    local.wait()
    half_all = buf.at[pl.ds(0, 4 * nz)]
    got(half_all, cs.at[1])

    for l in range(2):
        packed = buf[pl.ds(l * 4 * nz, 4 * nz), pl.ds(dm.off_up, 16), :].astype(F32)
        up[l] = packed[:, :8, :].reshape(hv, 128).astype(BF16)

    tokens = dm.rows

    def block(l, k, off):
        return buf[pl.ds(l * 4 * nz + 4 * k, 4), pl.ds(off, 64), :].reshape(256, 128)

    def w_in(l, k):
        return jnp.concatenate([block(l, k, 64 * b) for b in range(hb)] + [block(l, k, dm.off_down)], axis=1)

    def w_back(l, k):
        return jnp.concatenate([block(l, k, dm.off_out + 64 * b) for b in range(hb)], axis=1)

    def cols(k):
        return pl.ds(256 * k, 256)

    width = d_all // PIECES
    per_piece = nz // PIECES

    def piece(ref, i, u, p):
        return ref.at[i, u, :, pl.ds(width * p, width)]

    def lanes(v):
        return v[:, :128] + v[:, 128:]

    def run_forward(u):
        for l in range(2):
            total = jnp.zeros((tokens, 128), F32)
            acc = jnp.zeros((tokens, hv + 128), F32)
            for p in range(PIECES):
                if l == 0:

                    @pl.when(x > 0)
                    def _(p=p):
                        got(piece(xs, 0, u, p), fr.at[u, p])

                for k in range(p * per_piece, (p + 1) * per_piece):
                    v = xs[l, u, :, cols(k)]
                    acc = acc + dot(v, w_in(l, k))
                    v = v.astype(F32)
                    total = total + lanes(v * v)
            inv = lax.rsqrt(jnp.sum(total, axis=-1, keepdims=True) * (1.0 / d_all) + EPS)
            iv[l, u] = jnp.broadcast_to(inv, (tokens, 128))
            raw[l, u] = acc
            acc = acc * inv
            low = acc[:, hv:].astype(BF16)
            lo[l, u] = low
            val = (acc[:, :hv] + dot_nt(low, up[l])).astype(BF16)

            def outputs(l=l, val=val):
                for p in range(PIECES):
                    for k in range(p * per_piece, (p + 1) * per_piece):
                        o = xs[l, u, :, cols(k)].astype(F32) + dot_nt(val, w_back(l, k))
                        xs[l + 1, u, :, cols(k)] = o.astype(BF16)
                    if l == 1:
                        for q in (p - 1,) if p < PIECES - 1 else (p - 1, p):
                            if q >= 0:
                                send(piece(xs, 2, u, q), piece(xs, 0, u, q), fs.at[u, q], fr.at[u, q], d_xp)

            if l == 0:
                outputs()
            else:
                pl.when(x < nx - 1)(outputs)

    def adapter_side(l, u, acc):
        dvb = acc.astype(BF16)
        dv[l, u] = dvb
        dlb = dot(dvb, up[l]).astype(BF16)
        dl[l, u] = dlb
        return jnp.concatenate([dvb, dlb], axis=1)

    def ahead(u, carry):
        acc = jnp.zeros((tokens, hv), F32)
        for k in range(nz):
            acc = acc + dot(gs[2, u, :, cols(k)], w_back(1, k))
        both = adapter_side(1, u, acc)
        for k in range(nz):
            pre[u, :, cols(k)] = dot_nt(both, w_in(1, k))
        return carry

    @pl.when(x == nx - 1)
    def _():
        lax.fori_loop(0, 3, ahead, 0)

    def input_grad(l, u, both, product, after):
        mean = jnp.sum(both.astype(F32) * raw[l, u], axis=-1, keepdims=True) * (1.0 / d_all)
        inv = iv[l, u][:, :1]
        scale = inv * inv * mean
        for p in range(PIECES):
            for k in range(p * per_piece, (p + 1) * per_piece):
                g = product(k) - xs[l, u, :, cols(k)].astype(F32) * scale
                gs[l, u, :, cols(k)] = (gs[l + 1, u, :, cols(k)].astype(F32) + inv * g).astype(BF16)
            after(p)

    def hand_out(l, u):
        @pl.when(yh == l)
        def _():
            pltpu.make_async_copy(gs.at[l, u], out.at[3 * yh + u], os.at[0, u]).start()

        @pl.when(yh != l)
        def _():
            send(gs.at[l, u], out.at[3 * yh + u], os.at[1, u], os.at[2, u], d_yo)

    def run_backward(u):
        @pl.when(x == nx - 1)
        def _():
            both = jnp.concatenate([dv[1, u], dl[1, u]], axis=1)
            input_grad(1, u, both, lambda k: pre[u, :, cols(k)], lambda p: None)

        @pl.when(x < nx - 1)
        def _():
            acc = jnp.zeros((tokens, hv), F32)
            for p in range(PIECES):
                got(piece(gs, 2, u, p), br.at[u, p])
                for k in range(p * per_piece, (p + 1) * per_piece):
                    acc = acc + dot(gs[2, u, :, cols(k)], w_back(1, k))
            both = adapter_side(1, u, acc)
            input_grad(1, u, both, lambda k: dot_nt(both, w_in(1, k)), lambda p: None)

        hand_out(1, u)
        acc = jnp.zeros((tokens, hv), F32)
        for k in range(nz):
            acc = acc + dot(gs[1, u, :, cols(k)], w_back(0, k))
        both = adapter_side(0, u, acc)

        def after(p):
            for q in (p - 1,) if p < PIECES - 1 else (p - 1, p):
                if q >= 0:

                    @pl.when(x > 0)
                    def _(q=q):
                        send(piece(gs, 0, u, q), piece(gs, 2, u, q), bs.at[u, q], br.at[u, q], d_xm)

        input_grad(0, u, both, lambda k: dot_nt(both, w_in(0, k)), after)
        hand_out(0, u)

    pad = jnp.zeros((128 - 3 * tokens, 128), BF16)

    def turn_normed():
        def layer(l, carry):
            inv = iv[l].reshape(3 * tokens, 128)[:, :1]
            for k in range(2 * nz):
                lane = pl.ds(128 * k, 128)
                n_k = xs[l, :, :, lane].reshape(3 * tokens, 128).astype(F32) * inv
                nt[l, lane, :] = jnp.concatenate([n_k.astype(BF16), pad], axis=0).T
            return carry

        lax.fori_loop(0, 2, layer, 0)

    last = x // (nx - 1)

    def turn(t, carry):
        u = last * ((t // 2) % 3) + (1 - last) * (t % 4)
        kind = last * (t % 2 + 2 * (t // 6)) + (1 - last) * (t // 4 + 2 * ((t % 4) // 3))

        @pl.when(kind == 0)
        def _():
            run_forward(u)

        @pl.when(kind == 1)
        def _():
            run_backward(u)

        @pl.when(kind == 2)
        def _():
            turn_normed()

        return carry

    lax.fori_loop(0, 7, turn, 0)

    def adapter_grads(l):
        dl_all = jnp.concatenate([dl[l].reshape(3 * tokens, 128), pad], axis=0)
        lo_all = lo[l].reshape(3 * tokens, 128)
        for k in range(nz):
            g = dot(nt[l, cols(k), :], dl_all).astype(BF16)
            for q in range(4):
                rr[2 * l + q // 2, k, q % 2, pl.ds(0, 64), :] = g[64 * q : 64 * q + 64]
        dv_all = dv[l].reshape(3 * tokens, hv)
        g = lax.dot_general(dv_all, lo_all, TN, preferred_element_type=F32).reshape(nz, 4, 8, 128)
        for q in range(4):
            g_q = g[:, q]
            padded = jnp.concatenate([g_q, jnp.zeros_like(g_q)], axis=1).astype(BF16)
            rr[2 * l + q // 2, :, q % 2, pl.ds(64, 16), :] = padded

    for l in range(2):
        adapter_grads(l)
        two = pl.ds(2 * l, 2)
        send(rr.at[two, :, 1 - c], rc.at[two], gsm.at[l, 0], gsm.at[l, 1], d_sib)

    halves = ((0, 48), (48, 32))
    steps = (nh - 2) // 2

    def at(way, dist):
        return (z + dist) % nz if way == 0 else (z + nz - dist) % nz

    def z_move(src, dst, h, way, j, dist):
        send(src, dst, zrr.at[0, h, way, j], zrr.at[1, h, way, j], dev(x, y, at(way, dist), c))

    lo_z, hi_z = pl.ds(0, nh), pl.ds(nh, nh)

    def rows_of(h):
        return pl.ds(*halves[h])

    for l in range(2):
        got(rc.at[pl.ds(2 * l, 2)], gsm.at[l, 1])
    for h in range(2):
        r = rows_of(h)

        def add_core(i, carry, r=r):
            s1[i, :, r, :] = (rr[i, :, c, r, :].astype(F32) + rc[i, :, r, :].astype(F32)).astype(BF16)
            return carry

        lax.fori_loop(0, NY, add_core, 0)
        send(s1.at[yo, lo_z, r, :], t1.at[:, r, :], gsm.at[h, 2], gsm.at[h, 3], d_yp)
        send(s1.at[yo, hi_z, r, :], t2.at[:, r, :], gsm.at[h, 4], gsm.at[h, 5], d_ym)
    for h in range(2):
        r = rows_of(h)
        got(t1.at[:, r, :], gsm.at[h, 3])
        s1[yp, lo_z, r, :] = (s1[yp, lo_z, r, :].astype(F32) + t1[:, r, :].astype(F32)).astype(BF16)
        got(t2.at[:, r, :], gsm.at[h, 5])
        s1[ym, hi_z, r, :] = (s1[ym, hi_z, r, :].astype(F32) + t2[:, r, :].astype(F32)).astype(BF16)
        send(s1.at[yp, :, r, :], v1.at[:, r, :], gsm.at[h, 6], gsm.at[h, 7], d_yp)
        send(s1.at[ym, :, r, :], v2.at[:, r, :], gsm.at[h, 8], gsm.at[h, 9], d_ym)
    for h in range(2):
        r = rows_of(h)
        got(v1.at[:, r, :], gsm.at[h, 7])
        got(v2.at[:, r, :], gsm.at[h, 9])
        total = s1[y, :, r, :].astype(F32) + v1[:, r, :].astype(F32) + v2[:, r, :].astype(F32)
        s2[:, r, :] = total.astype(BF16)

        for way in (0, 1):
            zs[way, 0, r, :] = s2[at(way, nh - 1), r, :]
            zs[way, 1, r, :] = s2[at(way, nh), r, :] if way == 0 else jnp.zeros((halves[h][1], 128), BF16)
            z_move(zs.at[way, :, r, :], zb.at[way, 0, :, r, :], h, way, 0, 2)

    for j in range(steps):
        for h in range(2):
            r = rows_of(h)
            for way in (0, 1):
                got(zb.at[way, j, :, r, :], zrr.at[1, h, way, j])
                for i in range(2):
                    mine = s2[at(way, nh - 3 - 2 * j + i), r, :].astype(F32)
                    zb[way, j, i, r, :] = (zb[way, j, i, r, :].astype(F32) + mine).astype(BF16)
                if j < steps - 1:
                    z_move(zb.at[way, j, :, r, :], zb.at[way, j + 1, :, r, :], h, way, j + 1, 2)
                else:
                    for i in range(2):
                        z_move(zb.at[way, j, i, r, :], zf.at[way, i, r, :], h, way, steps + i, i + 1)

    def z_sum(h):
        r = rows_of(h)
        acc = s2[z, r, :].astype(F32)
        for way in (0, 1):
            for i in range(2):
                got(zf.at[way, i, r, :], zrr.at[1, h, way, steps + i])
                acc = acc + zf[way, i, r, :].astype(F32)
        return acc

    top, bottom = z_sum(0), z_sum(1)
    gdown[pl.ds(0, 48)] = top
    gdown[pl.ds(48, 16)] = bottom[:16]
    gup[...] = bottom[16:24]

    left(half_all, cs.at[0])

    def span(n, r):
        return buf.at[pl.ds(0, n), pl.ds(0, r), :]

    left(span(nh, rows), ss.at[0])
    left(span(nh - 1, rows), ss.at[1])
    left(span(3 * (nh - 1), rp), ss.at[2])
    left(span(3 * nh, rp), ss.at[3])
    left(span(1, rows), ss.at[4])
    left(span(1, rows), ss.at[11])
    left(span(1, half), ss.at[5])
    left(span(1, rows - half), ss.at[6])
    left(span(nz - 1, rows - rp), ss.at[7])
    left(span(nz - 1, rows - rp), ss.at[8])
    left(span(nz - 1, qa - rp), ss.at[9])
    left(span(nz - 1, rows - qa), ss.at[10])
    for h in range(2):
        r = rows_of(h)
        for way in (0, 1):
            for j in range(steps):
                left(zs.at[way, :, r, :], zrr.at[0, h, way, j])
            for i in range(2):
                left(zf.at[way, i, r, :], zrr.at[0, h, way, steps + i])
        left(rc.at[pl.ds(2 * h, 2)], gsm.at[h, 0])
        left(t1.at[:, r, :], gsm.at[h, 2])
        left(t2.at[:, r, :], gsm.at[h, 4])
        left(v1.at[:, r, :], gsm.at[h, 6])
        left(v2.at[:, r, :], gsm.at[h, 8])
    for u in range(3):
        for p in range(PIECES):

            @pl.when(x < nx - 1)
            def _(u=u, p=p):
                left(piece(xs, 2, u, p), fs.at[u, p])

            @pl.when(x > 0)
            def _(u=u, p=p):
                left(piece(gs, 0, u, p), bs.at[u, p])

        pltpu.make_async_copy(gs.at[0, u], out.at[3 * yh + u], os.at[0, u]).wait()
        left(gs.at[0, u], os.at[1, u])
        got(out.at[3 * (1 - yh) + u], os.at[2, u])


def run_all(dm, order, wv, wo, ad, au, tok, cot):
    nz, d, hv, t = dm.nz, dm.d, dm.hv, dm.rows
    vm = pltpu.VMEM
    dma = pltpu.SemaphoreType.DMA
    in_vmem = pl.BlockSpec(memory_space=vm)
    anywhere = pl.BlockSpec(memory_space=pl.ANY)
    in_hbm = pl.BlockSpec(memory_space=pltpu.HBM)
    return pl.pallas_call(
        functools.partial(kernel, dm),
        out_shape=(
            jax.ShapeDtypeStruct((6, t, d), BF16),
            jax.ShapeDtypeStruct((64, 128), F32),
            jax.ShapeDtypeStruct((8, 128), F32),
        ),
        in_specs=[pl.BlockSpec(memory_space=pltpu.SMEM)] + [in_hbm] * 6,
        out_specs=(anywhere, in_vmem, in_vmem),
        scratch_shapes=[
            *(vm(a.shape, BF16) for a in (wv, wo, ad, au)),
            vm((dm.shard, 128), BF16),
            vm((6, t, d), BF16),
            vm((8 * nz, dm.shard, 128), BF16),
            vm((3, 3, t, d), BF16),
            vm((2, d, 128), BF16),
            vm((2, 3, t, 128), F32),
            vm((2, 3, t, hv + 128), F32),
            vm((3, t, d), F32),
            vm((2, 3, t, 128), BF16),
            vm((3, 3, t, d), BF16),
            vm((2, 3, t, hv), BF16),
            vm((2, 3, t, 128), BF16),
            vm((2, hv, 128), BF16),
            vm((4, nz, 2, 80, 128), BF16),
            vm((4, nz, 80, 128), BF16),
            vm((4, nz, 80, 128), BF16),
            vm((dm.nh, 80, 128), BF16),
            vm((dm.nh, 80, 128), BF16),
            vm((nz, 80, 128), BF16),
            vm((nz, 80, 128), BF16),
            vm((nz, 80, 128), BF16),
            vm((2, dm.nh // 2 - 1, 2, 80, 128), BF16),
            vm((2, 2, 80, 128), BF16),
            vm((2, 2, 80, 128), BF16),
            dma((4,)),
            dma((2, dm.nh + 2, 4)),
            dma((nz, 4)),
            dma((12,)),
            dma((4,)),
            dma((3, PIECES)),
            dma((3, PIECES)),
            dma((3, PIECES)),
            dma((3, PIECES)),
            dma((3, 3)),
            dma((2, 11)),
            dma((2, 2, 2, dm.nh // 2 + 1)),
        ],
        compiler_params=pltpu.CompilerParams(
            collective_id=0, has_side_effects=True, vmem_limit_bytes=62 * 1024 * 1024
        ),
        name="relay",
    )(order, wv, wo, ad, au, tok, cot)


def solution(mesh):
    def body(tokens, cotangent, order, w_value, w_out, adapter_down, adapter_up):
        dm = Dims(mesh, tokens.shape[1], tokens.shape[2], w_value.shape[2])
        dx, down, up = run_all(
            dm, order, w_value[0], w_out[0].T, adapter_down[0], adapter_up[0].T, tokens, cotangent
        )
        return (dx[None], down[None], up.T[None])

    return jax.shard_map(
        body,
        mesh=mesh,
        in_specs=(
            P(None, "fsdp", None),
            P(None, "fsdp", None),
            P(),
            P("section", "fsdp", None),
            P("section", None, "fsdp"),
            P("section", "fsdp", None),
            P("section", None, "fsdp"),
        ),
        out_specs=(
            P("section", None, "fsdp", None),
            P("section", "fsdp", None),
            P("section", None, "fsdp"),
        ),
        check_vma=False,
    )
```

```python
import functools

import jax
import jax.numpy as jnp
from jax import lax
from jax.experimental import pallas as pl
from jax.experimental.pallas import tpu as pltpu
from jax.sharding import PartitionSpec as P

EPS = 1e-05
MESH = pl.DeviceIdType.MESH
F32 = jnp.float32
BF16 = jnp.bfloat16
NT = (((1,), (1,)), ((), ()))
TN = (((0,), (0,)), ((), ()))
NY = 4
PIECES = 4


def dot(a, b):
    return jnp.dot(a, b, preferred_element_type=F32)


def dot_nt(a, b):
    return lax.dot_general(a, b, NT, preferred_element_type=F32)


class Dims:
    def __init__(self, mesh, rows, width, hv):
        self.nx = mesh.shape["section"] // 2
        self.nz = mesh.shape["fsdp"] // 4
        self.nh = self.nz // 2
        self.rows = rows
        self.d = width
        self.hv = hv
        self.hb = hv // 128
        self.off_out = 64 * self.hb
        self.off_down = 128 * self.hb
        self.off_up = self.off_down + 64
        self.shard = self.off_up + 16
        tiles = self.shard // 16
        self.rp = (tiles * 351 // 1000 + 1) * 16 if tiles < 37 else 208
        self.half = max((tiles + 1) // 2 * 16, self.rp)
        self.qa = self.rp + (tiles - self.rp // 16) // 2 * 16


def kernel(dm, order, wv_in, wo_in, ad_in, au_in, tok, cot, out, gdown, gup, wv, wo, ad, au, shard, stage, buf, xs, nt, iv, raw, pre, lo, gs, dv, dl,
           up, rr, rc, s1, t1, t2, v1, v2, s2, zb, zs, zf, ins, zr, yr, ss, cs, fr, fs, br, bs, os, gsm, zrr):
    nx, nz, nh, d_all, hv, hb = dm.nx, dm.nz, dm.nh, dm.d, dm.hv, dm.hb
    sec = lax.axis_index("section")
    fid = lax.axis_index("fsdp")
    x = sec // 2
    yh = sec % 2
    z = fid // 4
    y = yh * 2 + (fid // 2) % 2
    c = fid % 2
    yp, ym, yo = (y + 1) % NY, (y + NY - 1) % NY, (y + 2) % NY
    zp, zm = (z + 1) % nz, (z + nz - 1) % nz

    def dev(x_, y_, z_, c_):
        return (x_ * 2 + y_ // 2, z_ * 4 + (y_ % 2) * 2 + c_)

    def slot(y_, z_, c_):
        return (y_ // 2) * (4 * nz) + z_ * 4 + (y_ % 2) * 2 + c_

    d_zp, d_zm = dev(x, y, zp, c), dev(x, y, zm, c)
    d_yp, d_ym, d_yo = dev(x, yp, z, c), dev(x, ym, z, c), dev(x, yo, z, c)
    d_sib = dev(x, y, z, 1 - c)
    d_xp, d_xm = dev(x + 1, y, z, c), dev(x - 1, y, z, c)

    def send(src, dst, ssem, rsem, to):
        pltpu.make_async_remote_copy(
            src_ref=src, dst_ref=dst, send_sem=ssem, recv_sem=rsem, device_id=to, device_id_type=MESH
        ).start()

    def got(ref, rsem):
        pltpu.make_async_remote_copy(
            src_ref=ref, dst_ref=ref, send_sem=rsem, recv_sem=rsem, device_id=d_sib, device_id_type=MESH
        ).wait_recv()

    def left(ref, ssem):
        pltpu.make_async_remote_copy(
            src_ref=ref, dst_ref=ref, send_sem=ssem, recv_sem=ssem, device_id=d_sib, device_id_type=MESH
        ).wait_send()

    barrier = pltpu.get_barrier_semaphore()

    def greet(to):
        pl.semaphore_signal(barrier, inc=1, device_id=to, device_id_type=MESH)

    d_xs = dev((x + nx - 1) % nx, y, z, c), dev((x + 1) % nx, y, z, c)
    peers = (d_sib, d_yp, d_ym, d_zp, d_zm, *d_xs)
    for to in peers:
        greet(to)
    fetches = [
        pltpu.make_async_copy(src, dst, ins.at[i])
        for i, (src, dst) in enumerate(((wv_in, wv), (wo_in, wo), (ad_in, ad), (au_in, au)))
    ]
    for f in fetches:
        f.start()

    @pl.when(x == 0)
    def _():
        pltpu.make_async_copy(tok, stage, cs.at[3]).start()

    @pl.when(x == nx - 1)
    def _():
        pltpu.make_async_copy(cot, stage, cs.at[3]).start()

    for f in fetches:
        f.wait()
    for b in range(hb):
        shard[pl.ds(64 * b, 64)] = wv[:, 128 * b : 128 * b + 128]
        shard[pl.ds(dm.off_out + 64 * b, 64)] = wo[:, 128 * b : 128 * b + 128]
    shard[pl.ds(dm.off_down, 64)] = ad[...]
    turned = au[...].astype(F32)
    shard[pl.ds(dm.off_up, 16)] = jnp.concatenate([turned, jnp.zeros_like(turned)], axis=0).astype(BF16)

    pl.semaphore_wait(barrier, len(peers))

    rows, rp, half, qa = dm.shard, dm.rp, dm.half, dm.qa

    def part(s, r0, r1):
        return buf.at[s, pl.ds(r0, r1 - r0), :]

    def to_sib(s, r0, r1):
        send(part(s, r0, r1), part(s, r0, r1), cs.at[0], cs.at[1], d_sib)

    def move(s, r0, r1, ssem, rsem, to):
        send(part(s, r0, r1), part(s, r0, r1), ssem, rsem, to)

    me = slot(y, z, c)
    own = buf.at[me]
    send(shard, own, ss.at[0], zr.at[0, 1, 0], d_zp)
    send(shard, own, ss.at[1], zr.at[1, 1, 0], d_zm)
    send(shard, own, ss.at[4], yr.at[0, 0], d_yp)
    send(shard, own, ss.at[11], yr.at[0, 1], d_ym)
    send(shard, own, cs.at[0], cs.at[1], d_sib)
    local = pltpu.make_async_copy(shard, own, cs.at[2])
    local.start()

    @pl.when(x == 0)
    def _():
        pltpu.make_async_copy(tok, stage, cs.at[3]).wait()
        for u in range(3):
            xs[0, u] = stage[order[3 * yh + u]]

    @pl.when(x == nx - 1)
    def _():
        pltpu.make_async_copy(cot, stage, cs.at[3]).wait()
        for u in range(3):
            gs[2, u] = stage[order[3 * yh + u]]

    def send_p(s, kind, dist_of):
        for way, (ps, to) in enumerate(((2, d_zp), (3, d_zm))):
            move(s, 0, rp, ss.at[ps], zr.at[way, dist_of, kind], to)

    s_m, s_p, s_o = slot(ym, z, c), slot(yp, z, c), slot(yo, z, c)
    got(part(s_m, 0, rows), yr.at[0, 0])
    move(s_m, 0, half, ss.at[5], yr.at[0, 2], d_yp)
    send_p(s_m, 2, 1)
    to_sib(s_m, 0, rows)
    got(part(s_p, 0, rows), yr.at[0, 1])
    move(s_p, half, rows, ss.at[6], yr.at[0, 3], d_ym)
    send_p(s_p, 1, 1)
    to_sib(s_p, 0, rows)

    def z_from(way, d):
        return (z + nz - d) % nz if way == 0 else (z + d) % nz

    def e_of(way, d):
        return d if way == 0 else nh + d

    def limit(way):
        return nh if way == 0 else nh - 1

    def limit_p(way):
        return nh - 1 if way == 0 else nh

    def z_shard(way, d):
        s = slot(y, z_from(way, d), c)
        e = e_of(way, d)
        got(part(s, 0, rows), zr.at[way, d, 0])

        @pl.when(d < limit(way))
        def _():
            move(s, 0, rows, ss.at[way], zr.at[way, d + 1, 0], (d_zp, d_zm)[way])

        move(s, rp, rows, ss.at[7], yr.at[e, 0], d_yp)
        move(s, rp, rows, ss.at[8], yr.at[e, 1], d_ym)
        to_sib(s, 0, rows)

    def z_parts(way, d):
        for kind, col in ((2, ym), (1, yp), (3, yo)):
            s = slot(col, z_from(way, d), c)
            got(part(s, 0, rp), zr.at[way, d, kind])

            @pl.when(d < limit_p(way))
            def _(s=s, kind=kind):
                move(s, 0, rp, ss.at[2 + way], zr.at[way, d + 1, kind], (d_zp, d_zm)[way])

            to_sib(s, 0, rp)

    def y_near(way, d):
        e, zz = e_of(way, d), z_from(way, d)
        a, b = slot(ym, zz, c), slot(yp, zz, c)
        got(part(a, rp, rows), yr.at[e, 0])
        move(a, rp, qa, ss.at[9], yr.at[e, 2], d_yp)
        to_sib(a, rp, rows)
        got(part(b, rp, rows), yr.at[e, 1])
        move(b, qa, rows, ss.at[10], yr.at[e, 3], d_ym)
        to_sib(b, rp, rows)

    def y_far(way, d):
        e, zz = e_of(way, d), z_from(way, d)
        s = slot(yo, zz, c)
        got(part(s, rp, qa), yr.at[e, 2])
        to_sib(s, rp, qa)
        got(part(s, qa, rows), yr.at[e, 3])
        to_sib(s, qa, rows)

    def gather_step(d, carry):
        for way in (0, 1):
            pl.when(d <= limit(way))(functools.partial(z_shard, way, d))

        @pl.when(d == 1)
        def _():
            got(part(s_o, 0, half), yr.at[0, 2])
            send_p(s_o, 3, 1)
            to_sib(s_o, 0, half)
            got(part(s_o, half, rows), yr.at[0, 3])
            to_sib(s_o, half, rows)

        for way in (0, 1):
            pl.when(d <= limit_p(way))(functools.partial(z_parts, way, d))
        for way in (0, 1):
            pl.when((d > 1) & (d <= limit(way) + 1))(functools.partial(y_near, way, d - 1))
        for way in (0, 1):
            pl.when((d > 2) & (d <= limit(way) + 2))(functools.partial(y_far, way, d - 2))
        return carry

    lax.fori_loop(1, nh + 3, gather_step, 0)

    local.wait()
    half_all = buf.at[pl.ds(0, 4 * nz)]
    got(half_all, cs.at[1])

    for l in range(2):
        packed = buf[pl.ds(l * 4 * nz, 4 * nz), pl.ds(dm.off_up, 16), :].astype(F32)
        up[l] = packed[:, :8, :].reshape(hv, 128).astype(BF16)

    tokens = dm.rows

    def block(l, k, off):
        return buf[pl.ds(l * 4 * nz + 4 * k, 4), pl.ds(off, 64), :].reshape(256, 128)

    def w_in(l, k):
        return jnp.concatenate([block(l, k, 64 * b) for b in range(hb)] + [block(l, k, dm.off_down)], axis=1)

    def w_back(l, k):
        return jnp.concatenate([block(l, k, dm.off_out + 64 * b) for b in range(hb)], axis=1)

    def cols(k):
        return pl.ds(256 * k, 256)

    width = d_all // PIECES
    per_piece = nz // PIECES

    def piece(ref, i, u, p):
        return ref.at[i, u, :, pl.ds(width * p, width)]

    def lanes(v):
        return v[:, :128] + v[:, 128:]

    def run_forward(u):
        for l in range(2):
            total = jnp.zeros((tokens, 128), F32)
            acc = jnp.zeros((tokens, hv + 128), F32)
            for p in range(PIECES):
                if l == 0:

                    @pl.when(x > 0)
                    def _(p=p):
                        got(piece(xs, 0, u, p), fr.at[u, p])

                for k in range(p * per_piece, (p + 1) * per_piece):
                    v = xs[l, u, :, cols(k)]
                    acc = acc + dot(v, w_in(l, k))
                    v = v.astype(F32)
                    total = total + lanes(v * v)
            inv = lax.rsqrt(jnp.sum(total, axis=-1, keepdims=True) * (1.0 / d_all) + EPS)
            iv[l, u] = jnp.broadcast_to(inv, (tokens, 128))
            raw[l, u] = acc
            acc = acc * inv
            low = acc[:, hv:].astype(BF16)
            lo[l, u] = low
            val = (acc[:, :hv] + dot_nt(low, up[l])).astype(BF16)

            def outputs(l=l, val=val):
                for p in range(PIECES):
                    for k in range(p * per_piece, (p + 1) * per_piece):
                        o = xs[l, u, :, cols(k)].astype(F32) + dot_nt(val, w_back(l, k))
                        xs[l + 1, u, :, cols(k)] = o.astype(BF16)
                    if l == 1:
                        for q in (p - 1,) if p < PIECES - 1 else (p - 1, p):
                            if q >= 0:
                                send(piece(xs, 2, u, q), piece(xs, 0, u, q), fs.at[u, q], fr.at[u, q], d_xp)

            if l == 0:
                outputs()
            else:
                pl.when(x < nx - 1)(outputs)

    def adapter_side(l, u, acc):
        dvb = acc.astype(BF16)
        dv[l, u] = dvb
        dlb = dot(dvb, up[l]).astype(BF16)
        dl[l, u] = dlb
        return jnp.concatenate([dvb, dlb], axis=1)

    def ahead(u, carry):
        acc = jnp.zeros((tokens, hv), F32)
        for k in range(nz):
            acc = acc + dot(gs[2, u, :, cols(k)], w_back(1, k))
        both = adapter_side(1, u, acc)
        for k in range(nz):
            pre[u, :, cols(k)] = dot_nt(both, w_in(1, k))
        return carry

    @pl.when(x == nx - 1)
    def _():
        lax.fori_loop(0, 3, ahead, 0)

    def input_grad(l, u, both, product, after):
        mean = jnp.sum(both.astype(F32) * raw[l, u], axis=-1, keepdims=True) * (1.0 / d_all)
        inv = iv[l, u][:, :1]
        scale = inv * inv * mean
        for p in range(PIECES):
            for k in range(p * per_piece, (p + 1) * per_piece):
                g = product(k) - xs[l, u, :, cols(k)].astype(F32) * scale
                gs[l, u, :, cols(k)] = (gs[l + 1, u, :, cols(k)].astype(F32) + inv * g).astype(BF16)
            after(p)

    def hand_out(l, u):
        @pl.when(yh == l)
        def _():
            pltpu.make_async_copy(gs.at[l, u], out.at[3 * yh + u], os.at[0, u]).start()

        @pl.when((yh != l) & (u < 2))
        def _():
            send(gs.at[l, u], out.at[3 * yh + u], os.at[1, u], os.at[2, u], d_yo)

    def run_backward(u):
        @pl.when(x == nx - 1)
        def _():
            both = jnp.concatenate([dv[1, u], dl[1, u]], axis=1)
            input_grad(1, u, both, lambda k: pre[u, :, cols(k)], lambda p: None)

        @pl.when(x < nx - 1)
        def _():
            acc = jnp.zeros((tokens, hv), F32)
            for p in range(PIECES):
                got(piece(gs, 2, u, p), br.at[u, p])
                for k in range(p * per_piece, (p + 1) * per_piece):
                    acc = acc + dot(gs[2, u, :, cols(k)], w_back(1, k))
            both = adapter_side(1, u, acc)
            input_grad(1, u, both, lambda k: dot_nt(both, w_in(1, k)), lambda p: None)

        hand_out(1, u)
        acc = jnp.zeros((tokens, hv), F32)
        for k in range(nz):
            acc = acc + dot(gs[1, u, :, cols(k)], w_back(0, k))
        both = adapter_side(0, u, acc)

        def after(p):
            for q in (p - 1,) if p < PIECES - 1 else (p - 1, p):
                if q >= 0:

                    @pl.when(x > 0)
                    def _(q=q):
                        send(piece(gs, 0, u, q), piece(gs, 2, u, q), bs.at[u, q], br.at[u, q], d_xm)

        input_grad(0, u, both, lambda k: dot_nt(both, w_in(0, k)), after)
        hand_out(0, u)

    pad = jnp.zeros((128 - 3 * tokens, 128), BF16)

    def turn_normed():
        def layer(l, carry):
            inv = iv[l].reshape(3 * tokens, 128)[:, :1]
            for k in range(2 * nz):
                lane = pl.ds(128 * k, 128)
                n_k = xs[l, :, :, lane].reshape(3 * tokens, 128).astype(F32) * inv
                nt[l, lane, :] = jnp.concatenate([n_k.astype(BF16), pad], axis=0).T
            return carry

        lax.fori_loop(0, 2, layer, 0)

    last = x // (nx - 1)

    def turn(t, carry):
        u = last * ((t // 2) % 3) + (1 - last) * (t % 4)
        kind = last * (t % 2 + 2 * (t // 6)) + (1 - last) * (t // 4 + 2 * ((t % 4) // 3))

        @pl.when(kind == 0)
        def _():
            run_forward(u)

        @pl.when(kind == 1)
        def _():
            run_backward(u)

        @pl.when(kind == 2)
        def _():
            turn_normed()

        return carry

    lax.fori_loop(0, 7, turn, 0)

    def adapter_grads(l):
        dl_all = jnp.concatenate([dl[l].reshape(3 * tokens, 128), pad], axis=0)
        lo_all = lo[l].reshape(3 * tokens, 128)
        for k in range(nz):
            g = dot(nt[l, cols(k), :], dl_all).astype(BF16)
            for q in range(4):
                rr[2 * l + q // 2, k, q % 2, pl.ds(0, 64), :] = g[64 * q : 64 * q + 64]
        dv_all = dv[l].reshape(3 * tokens, hv)
        g = lax.dot_general(dv_all, lo_all, TN, preferred_element_type=F32).reshape(nz, 4, 8, 128)
        for q in range(4):
            g_q = g[:, q]
            padded = jnp.concatenate([g_q, jnp.zeros_like(g_q)], axis=1).astype(BF16)
            rr[2 * l + q // 2, :, q % 2, pl.ds(64, 16), :] = padded

    for l in range(2):
        adapter_grads(l)
        two = pl.ds(2 * l, 2)
        send(rr.at[two, :, 1 - c], rc.at[two], gsm.at[l, 0], gsm.at[l, 1], d_sib)

    halves = ((0, 48), (48, 32))
    steps = (nh - 2) // 2

    def at(way, dist):
        return (z + dist) % nz if way == 0 else (z + nz - dist) % nz

    def z_move(src, dst, h, way, j, dist):
        send(src, dst, zrr.at[0, h, way, j], zrr.at[1, h, way, j], dev(x, y, at(way, dist), c))

    lo_z, hi_z = pl.ds(0, nh), pl.ds(nh, nh)

    def rows_of(h):
        return pl.ds(*halves[h])

    for l in range(2):
        got(rc.at[pl.ds(2 * l, 2)], gsm.at[l, 1])
    for h in range(2):
        r = rows_of(h)

        def add_core(i, carry, r=r):
            s1[i, :, r, :] = (rr[i, :, c, r, :].astype(F32) + rc[i, :, r, :].astype(F32)).astype(BF16)
            return carry

        lax.fori_loop(0, NY, add_core, 0)
        send(s1.at[yo, lo_z, r, :], t1.at[:, r, :], gsm.at[h, 2], gsm.at[h, 3], d_yp)
        send(s1.at[yo, hi_z, r, :], t2.at[:, r, :], gsm.at[h, 4], gsm.at[h, 5], d_ym)
    for h in range(2):
        r = rows_of(h)
        got(t1.at[:, r, :], gsm.at[h, 3])
        s1[yp, lo_z, r, :] = (s1[yp, lo_z, r, :].astype(F32) + t1[:, r, :].astype(F32)).astype(BF16)
        got(t2.at[:, r, :], gsm.at[h, 5])
        s1[ym, hi_z, r, :] = (s1[ym, hi_z, r, :].astype(F32) + t2[:, r, :].astype(F32)).astype(BF16)
        send(s1.at[yp, :, r, :], v1.at[:, r, :], gsm.at[h, 6], gsm.at[h, 7], d_yp)
        send(s1.at[ym, :, r, :], v2.at[:, r, :], gsm.at[h, 8], gsm.at[h, 9], d_ym)
    for l in range(2):

        @pl.when(yh != l)
        def _(l=l):
            send(gs.at[l, 2], out.at[3 * yh + 2], os.at[1, 2], os.at[2, 2], d_yo)

    for h in range(2):
        r = rows_of(h)
        got(v1.at[:, r, :], gsm.at[h, 7])
        got(v2.at[:, r, :], gsm.at[h, 9])
        total = s1[y, :, r, :].astype(F32) + v1[:, r, :].astype(F32) + v2[:, r, :].astype(F32)
        s2[:, r, :] = total.astype(BF16)

        for way in (0, 1):
            zs[way, 0, r, :] = s2[at(way, nh - 1), r, :]
            zs[way, 1, r, :] = s2[at(way, nh), r, :] if way == 0 else jnp.zeros((halves[h][1], 128), BF16)
            z_move(zs.at[way, :, r, :], zb.at[way, 0, :, r, :], h, way, 0, 2)

    for j in range(steps):
        for h in range(2):
            r = rows_of(h)
            for way in (0, 1):
                got(zb.at[way, j, :, r, :], zrr.at[1, h, way, j])
                for i in range(2):
                    mine = s2[at(way, nh - 3 - 2 * j + i), r, :].astype(F32)
                    zb[way, j, i, r, :] = (zb[way, j, i, r, :].astype(F32) + mine).astype(BF16)
                if j < steps - 1:
                    z_move(zb.at[way, j, :, r, :], zb.at[way, j + 1, :, r, :], h, way, j + 1, 2)
                else:
                    for i in range(2):
                        z_move(zb.at[way, j, i, r, :], zf.at[way, i, r, :], h, way, steps + i, i + 1)

    def z_sum(h):
        r = rows_of(h)
        acc = s2[z, r, :].astype(F32)
        for way in (0, 1):
            for i in range(2):
                got(zf.at[way, i, r, :], zrr.at[1, h, way, steps + i])
                acc = acc + zf[way, i, r, :].astype(F32)
        return acc

    top, bottom = z_sum(0), z_sum(1)
    gdown[pl.ds(0, 48)] = top
    gdown[pl.ds(48, 16)] = bottom[:16]
    gup[...] = bottom[16:24]

    left(half_all, cs.at[0])

    def span(n, r):
        return buf.at[pl.ds(0, n), pl.ds(0, r), :]

    left(span(nh, rows), ss.at[0])
    left(span(nh - 1, rows), ss.at[1])
    left(span(3 * (nh - 1), rp), ss.at[2])
    left(span(3 * nh, rp), ss.at[3])
    left(span(1, rows), ss.at[4])
    left(span(1, rows), ss.at[11])
    left(span(1, half), ss.at[5])
    left(span(1, rows - half), ss.at[6])
    left(span(nz - 1, rows - rp), ss.at[7])
    left(span(nz - 1, rows - rp), ss.at[8])
    left(span(nz - 1, qa - rp), ss.at[9])
    left(span(nz - 1, rows - qa), ss.at[10])
    for h in range(2):
        r = rows_of(h)
        for way in (0, 1):
            for j in range(steps):
                left(zs.at[way, :, r, :], zrr.at[0, h, way, j])
            for i in range(2):
                left(zf.at[way, i, r, :], zrr.at[0, h, way, steps + i])
        left(rc.at[pl.ds(2 * h, 2)], gsm.at[h, 0])
        left(t1.at[:, r, :], gsm.at[h, 2])
        left(t2.at[:, r, :], gsm.at[h, 4])
        left(v1.at[:, r, :], gsm.at[h, 6])
        left(v2.at[:, r, :], gsm.at[h, 8])
    for u in range(3):
        for p in range(PIECES):

            @pl.when(x < nx - 1)
            def _(u=u, p=p):
                left(piece(xs, 2, u, p), fs.at[u, p])

            @pl.when(x > 0)
            def _(u=u, p=p):
                left(piece(gs, 0, u, p), bs.at[u, p])

        pltpu.make_async_copy(gs.at[0, u], out.at[3 * yh + u], os.at[0, u]).wait()
        left(gs.at[0, u], os.at[1, u])
        got(out.at[3 * (1 - yh) + u], os.at[2, u])


def run_all(dm, order, wv, wo, ad, au, tok, cot):
    nz, d, hv, t = dm.nz, dm.d, dm.hv, dm.rows
    vm = pltpu.VMEM
    dma = pltpu.SemaphoreType.DMA
    in_vmem = pl.BlockSpec(memory_space=vm)
    anywhere = pl.BlockSpec(memory_space=pl.ANY)
    in_hbm = pl.BlockSpec(memory_space=pltpu.HBM)
    return pl.pallas_call(
        functools.partial(kernel, dm),
        out_shape=(
            jax.ShapeDtypeStruct((6, t, d), BF16),
            jax.ShapeDtypeStruct((64, 128), F32),
            jax.ShapeDtypeStruct((8, 128), F32),
        ),
        in_specs=[pl.BlockSpec(memory_space=pltpu.SMEM)] + [in_hbm] * 6,
        out_specs=(anywhere, in_vmem, in_vmem),
        scratch_shapes=[
            *(vm(a.shape, BF16) for a in (wv, wo, ad, au)),
            vm((dm.shard, 128), BF16),
            vm((6, t, d), BF16),
            vm((8 * nz, dm.shard, 128), BF16),
            vm((3, 3, t, d), BF16),
            vm((2, d, 128), BF16),
            vm((2, 3, t, 128), F32),
            vm((2, 3, t, hv + 128), F32),
            vm((3, t, d), F32),
            vm((2, 3, t, 128), BF16),
            vm((3, 3, t, d), BF16),
            vm((2, 3, t, hv), BF16),
            vm((2, 3, t, 128), BF16),
            vm((2, hv, 128), BF16),
            vm((4, nz, 2, 80, 128), BF16),
            vm((4, nz, 80, 128), BF16),
            vm((4, nz, 80, 128), BF16),
            vm((dm.nh, 80, 128), BF16),
            vm((dm.nh, 80, 128), BF16),
            vm((nz, 80, 128), BF16),
            vm((nz, 80, 128), BF16),
            vm((nz, 80, 128), BF16),
            vm((2, dm.nh // 2 - 1, 2, 80, 128), BF16),
            vm((2, 2, 80, 128), BF16),
            vm((2, 2, 80, 128), BF16),
            dma((4,)),
            dma((2, dm.nh + 2, 4)),
            dma((nz, 4)),
            dma((12,)),
            dma((4,)),
            dma((3, PIECES)),
            dma((3, PIECES)),
            dma((3, PIECES)),
            dma((3, PIECES)),
            dma((3, 3)),
            dma((2, 11)),
            dma((2, 2, 2, dm.nh // 2 + 1)),
        ],
        compiler_params=pltpu.CompilerParams(
            collective_id=0, has_side_effects=True, vmem_limit_bytes=62 * 1024 * 1024
        ),
        name="relay",
    )(order, wv, wo, ad, au, tok, cot)


def solution(mesh):
    def body(tokens, cotangent, order, w_value, w_out, adapter_down, adapter_up):
        dm = Dims(mesh, tokens.shape[1], tokens.shape[2], w_value.shape[2])
        dx, down, up = run_all(
            dm, order, w_value[0], w_out[0].T, adapter_down[0], adapter_up[0].T, tokens, cotangent
        )
        return (dx[None], down[None], up.T[None])

    return jax.shard_map(
        body,
        mesh=mesh,
        in_specs=(
            P(None, "fsdp", None),
            P(None, "fsdp", None),
            P(),
            P("section", "fsdp", None),
            P("section", None, "fsdp"),
            P("section", "fsdp", None),
            P("section", None, "fsdp"),
        ),
        out_specs=(
            P("section", None, "fsdp", None),
            P("section", "fsdp", None),
            P("section", None, "fsdp"),
        ),
        check_vma=False,
    )
```

```python
import functools

import jax
import jax.numpy as jnp
from jax import lax
from jax.experimental import pallas as pl
from jax.experimental.pallas import tpu as pltpu
from jax.sharding import PartitionSpec as P

EPS = 1e-05
MESH = pl.DeviceIdType.MESH
F32 = jnp.float32
BF16 = jnp.bfloat16
NT = (((1,), (1,)), ((), ()))
TN = (((0,), (0,)), ((), ()))
NY = 4
PIECES = 8
LANDING = 2


def dot(a, b):
    return jnp.dot(a, b, preferred_element_type=F32)


def dot_nt(a, b):
    return lax.dot_general(a, b, NT, preferred_element_type=F32)


class Dims:
    def __init__(self, mesh, rows, width, hv):
        self.nx = mesh.shape["section"] // 2
        self.nz = mesh.shape["fsdp"] // 4
        self.nh = self.nz // 2
        self.rows = rows
        self.d = width
        self.hv = hv
        self.hb = hv // 128
        self.off_out = 64 * self.hb
        self.off_down = 128 * self.hb
        self.off_up = self.off_down + 64
        self.shard = self.off_up + 16
        tiles = self.shard // 16
        self.rp = (tiles * 351 // 1000 + 1) * 16 if tiles < 37 else 208
        self.half = max((tiles + 1) // 2 * 16, self.rp)
        self.qa = self.rp + (tiles - self.rp // 16) // 2 * 16


def kernel(dm, order, wv_in, wo_in, ad_in, au_in, tok, cot, out, gdown, gup, wv, wo, ad, au, shard, stage, buf, xs, nt, iv, raw, pre, lo, gs, dv, dl,
           up, rr, rc, s1, t1, t2, v1, v2, s2, zb, zs, zf, ins, zr, yr, ss, cs, fr, fs, br, bs, os, gsm, zrr):
    nx, nz, nh, d_all, hv, hb = dm.nx, dm.nz, dm.nh, dm.d, dm.hv, dm.hb
    sec = lax.axis_index("section")
    fid = lax.axis_index("fsdp")
    x = sec // 2
    yh = sec % 2
    z = fid // 4
    y = yh * 2 + (fid // 2) % 2
    c = fid % 2
    yp, ym, yo = (y + 1) % NY, (y + NY - 1) % NY, (y + 2) % NY
    zp, zm = (z + 1) % nz, (z + nz - 1) % nz

    def dev(x_, y_, z_, c_):
        return (x_ * 2 + y_ // 2, z_ * 4 + (y_ % 2) * 2 + c_)

    def slot(y_, z_, c_):
        return (y_ // 2) * (4 * nz) + z_ * 4 + (y_ % 2) * 2 + c_

    d_zp, d_zm = dev(x, y, zp, c), dev(x, y, zm, c)
    d_yp, d_ym, d_yo = dev(x, yp, z, c), dev(x, ym, z, c), dev(x, yo, z, c)
    d_sib = dev(x, y, z, 1 - c)
    d_xp, d_xm = dev(x + 1, y, z, c), dev(x - 1, y, z, c)

    def send(src, dst, ssem, rsem, to):
        pltpu.make_async_remote_copy(
            src_ref=src, dst_ref=dst, send_sem=ssem, recv_sem=rsem, device_id=to, device_id_type=MESH
        ).start()

    def got(ref, rsem):
        pltpu.make_async_remote_copy(
            src_ref=ref, dst_ref=ref, send_sem=rsem, recv_sem=rsem, device_id=d_sib, device_id_type=MESH
        ).wait_recv()

    def left(ref, ssem):
        pltpu.make_async_remote_copy(
            src_ref=ref, dst_ref=ref, send_sem=ssem, recv_sem=ssem, device_id=d_sib, device_id_type=MESH
        ).wait_send()

    barrier = pltpu.get_barrier_semaphore()

    def greet(to):
        pl.semaphore_signal(barrier, inc=1, device_id=to, device_id_type=MESH)

    d_xs = dev((x + nx - 1) % nx, y, z, c), dev((x + 1) % nx, y, z, c)
    peers = (d_sib, d_yp, d_ym, d_zp, d_zm, *d_xs)
    for to in peers:
        greet(to)
    fetches = [
        pltpu.make_async_copy(src, dst, ins.at[i])
        for i, (src, dst) in enumerate(((wv_in, wv), (wo_in, wo), (ad_in, ad), (au_in, au)))
    ]
    for f in fetches:
        f.start()

    @pl.when(x == 0)
    def _():
        pltpu.make_async_copy(tok, stage, cs.at[3]).start()

    @pl.when(x == nx - 1)
    def _():
        pltpu.make_async_copy(cot, stage, cs.at[3]).start()

    for f in fetches:
        f.wait()
    for b in range(hb):
        shard[pl.ds(64 * b, 64)] = wv[:, 128 * b : 128 * b + 128]
        shard[pl.ds(dm.off_out + 64 * b, 64)] = wo[:, 128 * b : 128 * b + 128]
    shard[pl.ds(dm.off_down, 64)] = ad[...]
    turned = au[...].astype(F32)
    shard[pl.ds(dm.off_up, 16)] = jnp.concatenate([turned, jnp.zeros_like(turned)], axis=0).astype(BF16)

    pl.semaphore_wait(barrier, len(peers))

    rows, rp, half, qa = dm.shard, dm.rp, dm.half, dm.qa

    def part(s, r0, r1):
        return buf.at[s, pl.ds(r0, r1 - r0), :]

    def to_sib(s, r0, r1):
        send(part(s, r0, r1), part(s, r0, r1), cs.at[0], cs.at[1], d_sib)

    def move(s, r0, r1, ssem, rsem, to):
        send(part(s, r0, r1), part(s, r0, r1), ssem, rsem, to)

    me = slot(y, z, c)
    own = buf.at[me]
    send(shard, own, ss.at[0], zr.at[0, 1, 0], d_zp)
    send(shard, own, ss.at[1], zr.at[1, 1, 0], d_zm)
    send(shard, own, ss.at[4], yr.at[0, 0], d_yp)
    send(shard, own, ss.at[11], yr.at[0, 1], d_ym)
    send(shard, own, cs.at[0], cs.at[1], d_sib)
    local = pltpu.make_async_copy(shard, own, cs.at[2])
    local.start()

    @pl.when(x == 0)
    def _():
        pltpu.make_async_copy(tok, stage, cs.at[3]).wait()
        for u in range(3):
            xs[0, u] = stage[order[3 * yh + u]]

    @pl.when(x == nx - 1)
    def _():
        pltpu.make_async_copy(cot, stage, cs.at[3]).wait()
        for u in range(3):
            gs[2, u] = stage[order[3 * yh + u]]

    def send_p(s, kind, dist_of):
        for way, (ps, to) in enumerate(((2, d_zp), (3, d_zm))):
            move(s, 0, rp, ss.at[ps], zr.at[way, dist_of, kind], to)

    s_m, s_p, s_o = slot(ym, z, c), slot(yp, z, c), slot(yo, z, c)
    got(part(s_m, 0, rows), yr.at[0, 0])
    move(s_m, 0, half, ss.at[5], yr.at[0, 2], d_yp)
    send_p(s_m, 2, 1)
    to_sib(s_m, 0, rows)
    got(part(s_p, 0, rows), yr.at[0, 1])
    move(s_p, half, rows, ss.at[6], yr.at[0, 3], d_ym)
    send_p(s_p, 1, 1)
    to_sib(s_p, 0, rows)

    def z_from(way, d):
        return (z + nz - d) % nz if way == 0 else (z + d) % nz

    def e_of(way, d):
        return d if way == 0 else nh + d

    def limit(way):
        return nh if way == 0 else nh - 1

    def limit_p(way):
        return nh - 1 if way == 0 else nh

    def z_shard(way, d):
        s = slot(y, z_from(way, d), c)
        e = e_of(way, d)
        got(part(s, 0, rows), zr.at[way, d, 0])

        @pl.when(d < limit(way))
        def _():
            move(s, 0, rows, ss.at[way], zr.at[way, d + 1, 0], (d_zp, d_zm)[way])

        move(s, rp, rows, ss.at[7], yr.at[e, 0], d_yp)
        move(s, rp, rows, ss.at[8], yr.at[e, 1], d_ym)
        to_sib(s, 0, rows)

    def z_parts(way, d):
        for kind, col in ((2, ym), (1, yp), (3, yo)):
            s = slot(col, z_from(way, d), c)
            got(part(s, 0, rp), zr.at[way, d, kind])

            @pl.when(d < limit_p(way))
            def _(s=s, kind=kind):
                move(s, 0, rp, ss.at[2 + way], zr.at[way, d + 1, kind], (d_zp, d_zm)[way])

            to_sib(s, 0, rp)

    def y_near(way, d):
        e, zz = e_of(way, d), z_from(way, d)
        a, b = slot(ym, zz, c), slot(yp, zz, c)
        got(part(a, rp, rows), yr.at[e, 0])
        move(a, rp, qa, ss.at[9], yr.at[e, 2], d_yp)
        to_sib(a, rp, rows)
        got(part(b, rp, rows), yr.at[e, 1])
        move(b, qa, rows, ss.at[10], yr.at[e, 3], d_ym)
        to_sib(b, rp, rows)

    def y_far(way, d):
        e, zz = e_of(way, d), z_from(way, d)
        s = slot(yo, zz, c)
        got(part(s, rp, qa), yr.at[e, 2])
        to_sib(s, rp, qa)
        got(part(s, qa, rows), yr.at[e, 3])
        to_sib(s, qa, rows)

    def gather_step(d, carry):
        for way in (0, 1):
            pl.when(d <= limit(way))(functools.partial(z_shard, way, d))

        @pl.when(d == 1)
        def _():
            got(part(s_o, 0, half), yr.at[0, 2])
            send_p(s_o, 3, 1)
            to_sib(s_o, 0, half)
            got(part(s_o, half, rows), yr.at[0, 3])
            to_sib(s_o, half, rows)

        for way in (0, 1):
            pl.when(d <= limit_p(way))(functools.partial(z_parts, way, d))
        for way in (0, 1):
            pl.when((d > 1) & (d <= limit(way) + 1))(functools.partial(y_near, way, d - 1))
        for way in (0, 1):
            pl.when((d > 2) & (d <= limit(way) + 2))(functools.partial(y_far, way, d - 2))
        return carry

    lax.fori_loop(1, nh + 3, gather_step, 0)

    local.wait()
    half_all = buf.at[pl.ds(0, 4 * nz)]
    got(half_all, cs.at[1])

    for l in range(2):
        packed = buf[pl.ds(l * 4 * nz, 4 * nz), pl.ds(dm.off_up, 16), :].astype(F32)
        up[l] = packed[:, :8, :].reshape(hv, 128).astype(BF16)

    tokens = dm.rows

    def block(l, k, off):
        return buf[pl.ds(l * 4 * nz + 4 * k, 4), pl.ds(off, 64), :].reshape(256, 128)

    def w_in(l, k):
        return jnp.concatenate([block(l, k, 64 * b) for b in range(hb)] + [block(l, k, dm.off_down)], axis=1)

    def w_back(l, k):
        return jnp.concatenate([block(l, k, dm.off_out + 64 * b) for b in range(hb)], axis=1)

    def cols(k):
        return pl.ds(256 * k, 256)

    width = d_all // PIECES
    per_piece = nz // PIECES

    def piece(ref, i, u, p):
        return ref.at[i, u, :, pl.ds(width * p, width)]

    def lanes(v):
        return v[:, :128] + v[:, 128:]

    def run_forward(u):
        for l in range(2):
            total = jnp.zeros((tokens, 128), F32)
            acc = jnp.zeros((tokens, hv + 128), F32)
            for p in range(0, PIECES, LANDING):
                if l == 0:

                    @pl.when(x > 0)
                    def _(p=p):
                        for q in range(p, p + LANDING):
                            got(piece(xs, 0, u, q), fr.at[u, q])

                for k in range(p * per_piece, (p + LANDING) * per_piece):
                    v = xs[l, u, :, cols(k)]
                    acc = acc + dot(v, w_in(l, k))
                    v = v.astype(F32)
                    total = total + lanes(v * v)
            inv = lax.rsqrt(jnp.sum(total, axis=-1, keepdims=True) * (1.0 / d_all) + EPS)
            iv[l, u] = jnp.broadcast_to(inv, (tokens, 128))
            raw[l, u] = acc
            acc = acc * inv
            low = acc[:, hv:].astype(BF16)
            lo[l, u] = low
            val = (acc[:, :hv] + dot_nt(low, up[l])).astype(BF16)

            def outputs(l=l, val=val):
                for p in range(PIECES):
                    for k in range(p * per_piece, (p + 1) * per_piece):
                        o = xs[l, u, :, cols(k)].astype(F32) + dot_nt(val, w_back(l, k))
                        xs[l + 1, u, :, cols(k)] = o.astype(BF16)
                    if l == 1:
                        for q in (p - 1,) if p < PIECES - 1 else (p - 1, p):
                            if q >= 0:
                                send(piece(xs, 2, u, q), piece(xs, 0, u, q), fs.at[u, q], fr.at[u, q], d_xp)

            if l == 0:
                outputs()
            else:
                pl.when(x < nx - 1)(outputs)

    def adapter_side(l, u, acc):
        dvb = acc.astype(BF16)
        dv[l, u] = dvb
        dlb = dot(dvb, up[l]).astype(BF16)
        dl[l, u] = dlb
        return jnp.concatenate([dvb, dlb], axis=1)

    def ahead(u, carry):
        acc = jnp.zeros((tokens, hv), F32)
        for k in range(nz):
            acc = acc + dot(gs[2, u, :, cols(k)], w_back(1, k))
        both = adapter_side(1, u, acc)
        for k in range(nz):
            pre[u, :, cols(k)] = dot_nt(both, w_in(1, k))
        return carry

    @pl.when(x == nx - 1)
    def _():
        lax.fori_loop(0, 3, ahead, 0)

    def input_grad(l, u, both, product, after):
        mean = jnp.sum(both.astype(F32) * raw[l, u], axis=-1, keepdims=True) * (1.0 / d_all)
        inv = iv[l, u][:, :1]
        scale = inv * inv * mean
        for p in range(PIECES):
            for k in range(p * per_piece, (p + 1) * per_piece):
                g = product(k) - xs[l, u, :, cols(k)].astype(F32) * scale
                gs[l, u, :, cols(k)] = (gs[l + 1, u, :, cols(k)].astype(F32) + inv * g).astype(BF16)
            after(p)

    def hand_out(l, u):
        @pl.when(yh == l)
        def _():
            pltpu.make_async_copy(gs.at[l, u], out.at[3 * yh + u], os.at[0, u]).start()

        @pl.when((yh != l) & (u < 2))
        def _():
            send(gs.at[l, u], out.at[3 * yh + u], os.at[1, u], os.at[2, u], d_yo)

    def run_backward(u):
        @pl.when(x == nx - 1)
        def _():
            both = jnp.concatenate([dv[1, u], dl[1, u]], axis=1)
            input_grad(1, u, both, lambda k: pre[u, :, cols(k)], lambda p: None)

        @pl.when(x < nx - 1)
        def _():
            acc = jnp.zeros((tokens, hv), F32)
            for p in range(0, PIECES, LANDING):
                for q in range(p, p + LANDING):
                    got(piece(gs, 2, u, q), br.at[u, q])
                for k in range(p * per_piece, (p + LANDING) * per_piece):
                    acc = acc + dot(gs[2, u, :, cols(k)], w_back(1, k))
            both = adapter_side(1, u, acc)
            input_grad(1, u, both, lambda k: dot_nt(both, w_in(1, k)), lambda p: None)

        hand_out(1, u)
        acc = jnp.zeros((tokens, hv), F32)
        for k in range(nz):
            acc = acc + dot(gs[1, u, :, cols(k)], w_back(0, k))
        both = adapter_side(0, u, acc)

        def after(p):
            for q in (p - 1,) if p < PIECES - 1 else (p - 1, p):
                if q >= 0:

                    @pl.when(x > 0)
                    def _(q=q):
                        send(piece(gs, 0, u, q), piece(gs, 2, u, q), bs.at[u, q], br.at[u, q], d_xm)

        input_grad(0, u, both, lambda k: dot_nt(both, w_in(0, k)), after)
        hand_out(0, u)

    pad = jnp.zeros((128 - 3 * tokens, 128), BF16)

    def turn_normed():
        def layer(l, carry):
            inv = iv[l].reshape(3 * tokens, 128)[:, :1]
            for k in range(2 * nz):
                lane = pl.ds(128 * k, 128)
                n_k = xs[l, :, :, lane].reshape(3 * tokens, 128).astype(F32) * inv
                nt[l, lane, :] = jnp.concatenate([n_k.astype(BF16), pad], axis=0).T
            return carry

        lax.fori_loop(0, 2, layer, 0)

    last = x // (nx - 1)

    def turn(t, carry):
        u = last * ((t // 2) % 3) + (1 - last) * (t % 4)
        kind = last * (t % 2 + 2 * (t // 6)) + (1 - last) * (t // 4 + 2 * ((t % 4) // 3))

        @pl.when(kind == 0)
        def _():
            run_forward(u)

        @pl.when(kind == 1)
        def _():
            run_backward(u)

        @pl.when(kind == 2)
        def _():
            turn_normed()

        return carry

    lax.fori_loop(0, 7, turn, 0)

    def adapter_grads(l):
        dl_all = jnp.concatenate([dl[l].reshape(3 * tokens, 128), pad], axis=0)
        lo_all = lo[l].reshape(3 * tokens, 128)
        for k in range(nz):
            g = dot(nt[l, cols(k), :], dl_all).astype(BF16)
            for q in range(4):
                rr[2 * l + q // 2, k, q % 2, pl.ds(0, 64), :] = g[64 * q : 64 * q + 64]
        dv_all = dv[l].reshape(3 * tokens, hv)
        g = lax.dot_general(dv_all, lo_all, TN, preferred_element_type=F32).reshape(nz, 4, 8, 128)
        for q in range(4):
            g_q = g[:, q]
            padded = jnp.concatenate([g_q, jnp.zeros_like(g_q)], axis=1).astype(BF16)
            rr[2 * l + q // 2, :, q % 2, pl.ds(64, 16), :] = padded

    for l in range(2):
        adapter_grads(l)
        two = pl.ds(2 * l, 2)
        send(rr.at[two, :, 1 - c], rc.at[two], gsm.at[l, 0], gsm.at[l, 1], d_sib)

    halves = ((0, 48), (48, 32))
    steps = (nh - 2) // 2

    def at(way, dist):
        return (z + dist) % nz if way == 0 else (z + nz - dist) % nz

    def z_move(src, dst, h, way, j, dist):
        send(src, dst, zrr.at[0, h, way, j], zrr.at[1, h, way, j], dev(x, y, at(way, dist), c))

    lo_z, hi_z = pl.ds(0, nh), pl.ds(nh, nh)

    def rows_of(h):
        return pl.ds(*halves[h])

    for l in range(2):
        got(rc.at[pl.ds(2 * l, 2)], gsm.at[l, 1])
    for h in range(2):
        r = rows_of(h)

        def add_core(i, carry, r=r):
            s1[i, :, r, :] = (rr[i, :, c, r, :].astype(F32) + rc[i, :, r, :].astype(F32)).astype(BF16)
            return carry

        lax.fori_loop(0, NY, add_core, 0)
        send(s1.at[yo, lo_z, r, :], t1.at[:, r, :], gsm.at[h, 2], gsm.at[h, 3], d_yp)
        send(s1.at[yo, hi_z, r, :], t2.at[:, r, :], gsm.at[h, 4], gsm.at[h, 5], d_ym)
    for h in range(2):
        r = rows_of(h)
        got(t1.at[:, r, :], gsm.at[h, 3])
        s1[yp, lo_z, r, :] = (s1[yp, lo_z, r, :].astype(F32) + t1[:, r, :].astype(F32)).astype(BF16)
        got(t2.at[:, r, :], gsm.at[h, 5])
        s1[ym, hi_z, r, :] = (s1[ym, hi_z, r, :].astype(F32) + t2[:, r, :].astype(F32)).astype(BF16)
        send(s1.at[yp, :, r, :], v1.at[:, r, :], gsm.at[h, 6], gsm.at[h, 7], d_yp)
        send(s1.at[ym, :, r, :], v2.at[:, r, :], gsm.at[h, 8], gsm.at[h, 9], d_ym)
    for l in range(2):

        @pl.when(yh != l)
        def _(l=l):
            send(gs.at[l, 2], out.at[3 * yh + 2], os.at[1, 2], os.at[2, 2], d_yo)

    for h in range(2):
        r = rows_of(h)
        got(v1.at[:, r, :], gsm.at[h, 7])
        got(v2.at[:, r, :], gsm.at[h, 9])
        total = s1[y, :, r, :].astype(F32) + v1[:, r, :].astype(F32) + v2[:, r, :].astype(F32)
        s2[:, r, :] = total.astype(BF16)

        for way in (0, 1):
            zs[way, 0, r, :] = s2[at(way, nh - 1), r, :]
            zs[way, 1, r, :] = s2[at(way, nh), r, :] if way == 0 else jnp.zeros((halves[h][1], 128), BF16)
            z_move(zs.at[way, :, r, :], zb.at[way, 0, :, r, :], h, way, 0, 2)

    for j in range(steps):
        for h in range(2):
            r = rows_of(h)
            for way in (0, 1):
                got(zb.at[way, j, :, r, :], zrr.at[1, h, way, j])
                for i in range(2):
                    mine = s2[at(way, nh - 3 - 2 * j + i), r, :].astype(F32)
                    zb[way, j, i, r, :] = (zb[way, j, i, r, :].astype(F32) + mine).astype(BF16)
                if j < steps - 1:
                    z_move(zb.at[way, j, :, r, :], zb.at[way, j + 1, :, r, :], h, way, j + 1, 2)
                else:
                    for i in range(2):
                        z_move(zb.at[way, j, i, r, :], zf.at[way, i, r, :], h, way, steps + i, i + 1)

    def z_sum(h):
        r = rows_of(h)
        acc = s2[z, r, :].astype(F32)
        for way in (0, 1):
            for i in range(2):
                got(zf.at[way, i, r, :], zrr.at[1, h, way, steps + i])
                acc = acc + zf[way, i, r, :].astype(F32)
        return acc

    top, bottom = z_sum(0), z_sum(1)
    gdown[pl.ds(0, 48)] = top
    gdown[pl.ds(48, 16)] = bottom[:16]
    gup[...] = bottom[16:24]

    left(half_all, cs.at[0])

    def span(n, r):
        return buf.at[pl.ds(0, n), pl.ds(0, r), :]

    left(span(nh, rows), ss.at[0])
    left(span(nh - 1, rows), ss.at[1])
    left(span(3 * (nh - 1), rp), ss.at[2])
    left(span(3 * nh, rp), ss.at[3])
    left(span(1, rows), ss.at[4])
    left(span(1, rows), ss.at[11])
    left(span(1, half), ss.at[5])
    left(span(1, rows - half), ss.at[6])
    left(span(nz - 1, rows - rp), ss.at[7])
    left(span(nz - 1, rows - rp), ss.at[8])
    left(span(nz - 1, qa - rp), ss.at[9])
    left(span(nz - 1, rows - qa), ss.at[10])
    for h in range(2):
        r = rows_of(h)
        for way in (0, 1):
            for j in range(steps):
                left(zs.at[way, :, r, :], zrr.at[0, h, way, j])
            for i in range(2):
                left(zf.at[way, i, r, :], zrr.at[0, h, way, steps + i])
        left(rc.at[pl.ds(2 * h, 2)], gsm.at[h, 0])
        left(t1.at[:, r, :], gsm.at[h, 2])
        left(t2.at[:, r, :], gsm.at[h, 4])
        left(v1.at[:, r, :], gsm.at[h, 6])
        left(v2.at[:, r, :], gsm.at[h, 8])
    for u in range(3):
        for p in range(PIECES):

            @pl.when(x < nx - 1)
            def _(u=u, p=p):
                left(piece(xs, 2, u, p), fs.at[u, p])

            @pl.when(x > 0)
            def _(u=u, p=p):
                left(piece(gs, 0, u, p), bs.at[u, p])

        pltpu.make_async_copy(gs.at[0, u], out.at[3 * yh + u], os.at[0, u]).wait()
        left(gs.at[0, u], os.at[1, u])
        got(out.at[3 * (1 - yh) + u], os.at[2, u])


def run_all(dm, order, wv, wo, ad, au, tok, cot):
    nz, d, hv, t = dm.nz, dm.d, dm.hv, dm.rows
    vm = pltpu.VMEM
    dma = pltpu.SemaphoreType.DMA
    in_vmem = pl.BlockSpec(memory_space=vm)
    anywhere = pl.BlockSpec(memory_space=pl.ANY)
    in_hbm = pl.BlockSpec(memory_space=pltpu.HBM)
    return pl.pallas_call(
        functools.partial(kernel, dm),
        out_shape=(
            jax.ShapeDtypeStruct((6, t, d), BF16),
            jax.ShapeDtypeStruct((64, 128), F32),
            jax.ShapeDtypeStruct((8, 128), F32),
        ),
        in_specs=[pl.BlockSpec(memory_space=pltpu.SMEM)] + [in_hbm] * 6,
        out_specs=(anywhere, in_vmem, in_vmem),
        scratch_shapes=[
            *(vm(a.shape, BF16) for a in (wv, wo, ad, au)),
            vm((dm.shard, 128), BF16),
            vm((6, t, d), BF16),
            vm((8 * nz, dm.shard, 128), BF16),
            vm((3, 3, t, d), BF16),
            vm((2, d, 128), BF16),
            vm((2, 3, t, 128), F32),
            vm((2, 3, t, hv + 128), F32),
            vm((3, t, d), F32),
            vm((2, 3, t, 128), BF16),
            vm((3, 3, t, d), BF16),
            vm((2, 3, t, hv), BF16),
            vm((2, 3, t, 128), BF16),
            vm((2, hv, 128), BF16),
            vm((4, nz, 2, 80, 128), BF16),
            vm((4, nz, 80, 128), BF16),
            vm((4, nz, 80, 128), BF16),
            vm((dm.nh, 80, 128), BF16),
            vm((dm.nh, 80, 128), BF16),
            vm((nz, 80, 128), BF16),
            vm((nz, 80, 128), BF16),
            vm((nz, 80, 128), BF16),
            vm((2, dm.nh // 2 - 1, 2, 80, 128), BF16),
            vm((2, 2, 80, 128), BF16),
            vm((2, 2, 80, 128), BF16),
            dma((4,)),
            dma((2, dm.nh + 2, 4)),
            dma((nz, 4)),
            dma((12,)),
            dma((4,)),
            dma((3, PIECES)),
            dma((3, PIECES)),
            dma((3, PIECES)),
            dma((3, PIECES)),
            dma((3, 3)),
            dma((2, 11)),
            dma((2, 2, 2, dm.nh // 2 + 1)),
        ],
        compiler_params=pltpu.CompilerParams(
            collective_id=0, has_side_effects=True, vmem_limit_bytes=62 * 1024 * 1024
        ),
        name="relay",
    )(order, wv, wo, ad, au, tok, cot)


def solution(mesh):
    def body(tokens, cotangent, order, w_value, w_out, adapter_down, adapter_up):
        dm = Dims(mesh, tokens.shape[1], tokens.shape[2], w_value.shape[2])
        dx, down, up = run_all(
            dm, order, w_value[0], w_out[0].T, adapter_down[0], adapter_up[0].T, tokens, cotangent
        )
        return (dx[None], down[None], up.T[None])

    return jax.shard_map(
        body,
        mesh=mesh,
        in_specs=(
            P(None, "fsdp", None),
            P(None, "fsdp", None),
            P(),
            P("section", "fsdp", None),
            P("section", None, "fsdp"),
            P("section", "fsdp", None),
            P("section", None, "fsdp"),
        ),
        out_specs=(
            P("section", None, "fsdp", None),
            P("section", "fsdp", None),
            P("section", None, "fsdp"),
        ),
        check_vma=False,
    )
```
